512 devices in a mesh: groups: 2 (over y), seq: 32 (over z), head: 4 (over x), rep: 2 (over core).
Axes of the slice: x: 4, y: 2, z: 32, core: 2. Of those that a mesh axis runs over, the one named last changes fastest.
The devices are a block of a 4x8x32 slice.
Arguments:
- tokens: bfloat16 [64, 4096], P('groups', ('seq', 'rep')), parts along dimension 0, may hold values from -6 to 6
- attn_gain: float32 [4096], P(('seq', 'rep')), may hold values from 0.25 to 1.75
- ffn_gain: float32 [4096], P(('seq', 'rep')), may hold values from 0.25 to 1.75
- w_query: bfloat16 [4096, 4096], P(('seq', 'rep'), 'head'), may hold values from -0.0625 to 0.0625
- w_key: bfloat16 [4096, 1024], P(('seq', 'rep'), 'head'), may hold values from -0.09375 to 0.09375
- w_value: bfloat16 [4096, 1024], P(('seq', 'rep'), 'head'), may hold values from -0.25 to 0.25
- w_out: bfloat16 [4096, 4096], P('head', ('seq', 'rep')), may hold values from -0.09375 to 0.09375
- w_gate: bfloat16 [4096, 7168], P(('seq', 'rep'), 'head'), may hold values from -0.09375 to 0.09375
- w_up: bfloat16 [4096, 7168], P(('seq', 'rep'), 'head'), may hold values from -0.09375 to 0.09375
- w_down: bfloat16 [7168, 4096], P('head', ('seq', 'rep')), may hold values from -0.0625 to 0.0625
- kv_pool: bfloat16 [2, 64, 32, 128, 1024], P(None, ('groups', 'seq'), 'head', 'rep'), parts along dimension 1, may hold values from -15 to 15
- lengths: int32 [64], P('groups'), parts along dimension 0, may hold values from 1 to 4096, 65536 in all
- pool_row: int32 [64], P('groups'), parts along dimension 0, may hold values from 0 to 31, each once
- block_table: int32 [64, 32], P('groups'), parts along dimension 0, may hold values from 0 to 31, each once within a row
Outputs:
- layer_out: bfloat16 [64, 4096], P('groups', ('seq', 'rep')), parts along dimension 0
- kv_decode: bfloat16 [2, 64, 4096, 1024], P(None, 'groups', ('seq', 'rep'), 'head'), parts along dimension 1
The draws below stay inside these ranges and needn't reach their ends.
There are 2 independent parts, one for each index of `groups`. The reference program is written for one: setup_inputs(seed, part) draws one part's arguments, and reference() takes and returns one part's arrays. A program takes and returns all parts, laid end to end along the dimension named above; an argument that names none is the same for every part. Nothing has to cross between parts.
Inputs may be any that keep to these rules, and one draw needn't show every extreme that they name: One sequence reaches 4096; the lengths sum to 65536. `pool_row`: a permutation of the pool rows. `block_table`: every row is a permutation of the 32 slots.
All inputs are finite; a program needn't handle non-finite values.
Results may differ from the reference program's by a relative error of at most 0.008.
Values may be sent and summed in bfloat16 or wider, within the bound.
A program may use at most 64 MiB of HBM per device.

```python
import math
import jax
import jax.numpy as jnp
import numpy as np
from jax import lax

D = 4096
H = 32
KVH = 8
HD = 128
FFW = 7168
BLK = 128
SEQS = 32
MAXBLK = 32
MAXLEN = 4096


def draw_tokens(key, part):
    values = jax.random.normal(key, (SEQS, D), jnp.float32)
    return jnp.clip(values, -6.0, 6.0).astype(jnp.bfloat16)


def draw_w_query(key, part):
    spread = D ** (-0.5)
    values = jax.random.normal(key, (D, H * HD), jnp.float32) * spread
    return jnp.clip(values, -4.0 * spread, 4.0 * spread).astype(jnp.bfloat16)


def draw_kv_pool(key, part):
    width = KVH * HD
    values = jax.random.normal(key, (2, SEQS, MAXBLK, BLK, width), jnp.float32) * 2.5
    return jnp.clip(values, -15.0, 15.0).astype(jnp.bfloat16)


def level_of(rng, dims, shards, low, high):
    def one(position, parts):
        heights = jax.random.uniform(jax.random.fold_in(jax.random.fold_in(rng, 6), position), (parts,), jnp.float32, low / len(shards), high / len(shards))
        return jnp.repeat(jnp.exp(heights), dims[position] // parts).reshape((-1,) + (1,) * (len(dims) - position - 1))

    factor_of = one(*shards[0])
    for cut in shards[1:]:
        factor_of = factor_of * one(*cut)
    return factor_of


def split_up(count, total, reach, slope):
    portions = [(1 << 20) // math.isqrt(rank ** slope) + 1 for rank in range(2, count + 1)]
    surplus, given = total - reach - (count - 1), [1] * (count - 1)
    while surplus > 0:
        movable = [i for i in range(count - 1) if given[i] < reach]
        mass, left = sum([portions[i] for i in movable]), surplus
        for i in movable:
            extra = min(reach - given[i], max(1, left * portions[i] // mass), surplus)
            given[i] = given[i] + extra
            surplus = surplus - extra
    return np.array([reach] + given)


def uneven(rng, count, total, limit, slope):
    if count == 2:
        one = jax.random.randint(rng, (), max(1, total - limit), min(limit, total - 1) + 1)
        return jnp.stack([one, total - one])
    tallies = jnp.asarray(split_up(count, total, limit, slope), jnp.int32)
    couples = (count - 1) // 2
    source_of, sink = tallies[1:1 + 2 * couples:2], tallies[2:2 + 2 * couples:2]
    margin = jnp.minimum(source_of - 1, limit - sink)
    passed = jax.random.randint(jax.random.fold_in(rng, 1), (couples,), 0, 1 << 20) % (margin + 1)
    tallies = tallies.at[1:1 + 2 * couples:2].set(source_of - passed).at[2:2 + 2 * couples:2].set(sink + passed)
    return tallies[jax.random.permutation(jax.random.fold_in(rng, 2), count)]


def bell_draw(own_key, dims, scale, limit, split=(), kind=jnp.bfloat16):
    entries = jax.random.normal(own_key, dims, jnp.float32) * scale
    if len(split) > 0:
        entries = level_of(own_key, dims, split, -0.22, 0.18) * entries
    return jnp.clip(entries, min=-limit, max=limit).astype(kind)


def setup_inputs(seed: int = 0, part: int = 0) -> dict:
    splits = jax.random.split(jax.random.key(seed), 15)
    own_keys = jax.random.split(jax.random.fold_in(splits[14], part), 15)
    return {
        "tokens": draw_tokens(jax.random.fold_in(jax.random.fold_in(splits[14], part), 71), part),
        "attn_gain": jnp.clip(1.0 + 0.15 * jax.random.normal(splits[1], (D,), jnp.float32), 0.25, 1.75),
        "ffn_gain": jnp.clip(1.0 + 0.15 * jax.random.normal(splits[2], (D,), jnp.float32), 0.25, 1.75),
        "w_query": draw_w_query(jax.random.fold_in(splits[14], 71), part),
        "w_key": bell_draw(splits[4], (D, KVH * HD), D ** -0.5, 0.09375, ((0, 64), (1, 4))),
        "w_value": bell_draw(splits[5], (D, KVH * HD), (D // 8) ** -0.5, 0.25, ((0, 64), (1, 4))),
        "w_out": bell_draw(splits[6], (H * HD, D), (H * HD) ** -0.5, 0.09375, ((0, 4), (1, 64))),
        "w_gate": bell_draw(splits[7], (D, FFW), D ** -0.5, 0.09375, ((0, 64), (1, 4))),
        "w_up": bell_draw(splits[8], (D, FFW), D ** -0.5, 0.09375, ((0, 64), (1, 4))),
        "w_down": bell_draw(splits[9], (FFW, D), FFW ** -0.5, 0.0625, ((0, 4), (1, 64))),
        "kv_pool": draw_kv_pool(jax.random.fold_in(jax.random.fold_in(splits[14], part), 71), part),
        "lengths": uneven(own_keys[11], SEQS, SEQS * MAXLEN // 2, MAXLEN, 2).astype(jnp.int32),
        "pool_row": jax.random.permutation(own_keys[12], SEQS).astype(jnp.int32),
        "block_table": jax.vmap(lambda own: jax.random.permutation(own, MAXBLK))(jax.random.split(own_keys[13], SEQS)).reshape((SEQS, MAXBLK)).astype(jnp.int32),
    }


EPSILON = 1e-05
ROPE_LOG = math.log(500000.0)
FLOOR_SCORE = -1e+30

def rms_scale(residual, gain):
    squares = lax.optimization_barrier(jnp.sum(residual * residual, axis=-1))
    return residual * lax.rsqrt(squares / D + EPSILON)[:, None] * gain

def rotate(values, positions):
    half_dim = values.shape[-1] // 2
    freq_table = jnp.exp(jnp.arange(half_dim, dtype=jnp.float32) * (-2.0 * ROPE_LOG / values.shape[-1]))
    angles = positions[:, None, None] * freq_table
    cosine = jnp.cos(angles)
    sine_part = jnp.sin(angles)
    first_half = values[..., :half_dim]
    second_half = values[..., half_dim:]
    return jnp.concatenate([first_half * cosine - second_half * sine_part, second_half * cosine + first_half * sine_part], axis=-1)

def reference(tokens, attn_gain, ffn_gain, w_query, w_key, w_value, w_out, w_gate, w_up, w_down, kv_pool, lengths, pool_row, block_table):
    residual = tokens.astype(jnp.float32)
    normed = rms_scale(residual, attn_gain).astype(jnp.bfloat16)
    queries = jnp.dot(normed, w_query, preferred_element_type=jnp.float32).reshape(SEQS, H, HD)
    keys_new = jnp.dot(normed, w_key, preferred_element_type=jnp.float32).reshape(SEQS, KVH, HD)
    values_new = jnp.dot(normed, w_value, preferred_element_type=jnp.float32).reshape(SEQS, KVH, HD)
    positions = lengths.astype(jnp.float32)
    rot_queries = rotate(queries, positions).astype(jnp.bfloat16)
    rot_keys = rotate(keys_new, positions).astype(jnp.bfloat16)
    new_values = values_new.astype(jnp.bfloat16)
    pool_rows = jnp.take(kv_pool, pool_row.astype(jnp.int32), axis=1)
    ordered = jax.vmap(lambda row_blocks, table_row: jnp.take(row_blocks, table_row, axis=1), in_axes=(1, 0), out_axes=1)(pool_rows, block_table.astype(jnp.int32))
    cache = ordered.reshape(2, SEQS, MAXLEN, KVH * HD)
    is_live = jnp.arange(MAXLEN, dtype=jnp.int32)[None, :] < lengths[:, None]
    kv_decode = jnp.where(is_live[None, :, :, None], cache, jnp.zeros((), jnp.bfloat16))
    factor = 1.0 / math.sqrt(HD)
    per_group = H // KVH

    def attend(record):
        query_row, key_own, value_own, key_rows, value_rows, usable = record
        query_f = query_row.astype(jnp.float32).reshape(KVH, per_group, HD)
        key_f = key_rows.astype(jnp.float32).reshape(MAXLEN, KVH, HD)
        value_f = value_rows.astype(jnp.float32).reshape(MAXLEN, KVH, HD)
        scores = jnp.einsum('ngd,tnd->ngt', query_f, key_f) * factor
        scores = jnp.where(usable[None, None, :], scores, FLOOR_SCORE)
        own_score = lax.optimization_barrier(jnp.sum(query_f * key_own.astype(jnp.float32)[:, None, :], axis=-1)) * factor
        largest = jnp.maximum(lax.optimization_barrier(jnp.max(scores, axis=-1)), own_score)
        weights = jnp.where(usable[None, None, :], jnp.exp(scores - largest[..., None]), 0.0)
        own_weight = jnp.exp(own_score - largest)
        denominator = lax.optimization_barrier(jnp.sum(weights, axis=-1)) + own_weight
        rounded = lax.optimization_barrier(weights.astype(jnp.bfloat16)).astype(jnp.float32)
        mixed = jnp.einsum('ngt,tnd->ngd', rounded, value_f) + own_weight[..., None] * value_own.astype(jnp.float32)[:, None, :]
        return (mixed / denominator[..., None]).reshape(H * HD)
    attn = lax.map(attend, (rot_queries, rot_keys, new_values, kv_decode[0], kv_decode[1], is_live)).astype(jnp.bfloat16)
    middle = residual + jnp.dot(attn, w_out, preferred_element_type=jnp.float32)
    normed_mid = rms_scale(middle, ffn_gain).astype(jnp.bfloat16)
    gate_sum = jnp.dot(normed_mid, w_gate, preferred_element_type=jnp.float32)
    up_sum = jnp.dot(normed_mid, w_up, preferred_element_type=jnp.float32)
    hidden = (jax.nn.silu(gate_sum) * up_sum).astype(jnp.bfloat16)
    layer_out = (middle + jnp.dot(hidden, w_down, preferred_element_type=jnp.float32)).astype(jnp.bfloat16)
    return (layer_out, kv_decode)
```

```python
import math

import jax
import jax.numpy as jnp
from jax import lax
from jax.sharding import PartitionSpec as P

D = 4096
H = 32
KVH = 8
HD = 128
BLK = 128
LANES = 128

EPSILON = 1e-05
ROPE_LOG = math.log(500000.0)
FLOOR_SCORE = -1e30


def exchanged(tiles, axis):
    return lax.all_to_all(tiles, axis, split_axis=0, concat_axis=0, tiled=True)


def from_everyone(value, axis):
    peers = lax.axis_size(axis)
    return exchanged(jnp.broadcast_to(value[None], (peers, *value.shape)), axis)


def rotate(values, position):
    half_dim = values.shape[-1] // 2
    freq_table = jnp.exp(
        jnp.arange(half_dim, dtype=jnp.float32) * (-2.0 * ROPE_LOG / values.shape[-1])
    )
    angles = position * freq_table
    cosine = jnp.cos(angles)
    sine_part = jnp.sin(angles)
    first_half = values[..., :half_dim]
    second_half = values[..., half_dim:]
    return jnp.concatenate(
        [
            first_half * cosine - second_half * sine_part,
            second_half * cosine + first_half * sine_part,
        ],
        axis=-1,
    )


def rows_to_owner(parts, squares, kind):
    rows = squares.shape[0]
    widths = [a.shape[2] for a in parts]
    extra = jnp.broadcast_to(squares[:, None, None], (rows, 2, LANES))
    tiles = jnp.concatenate([*parts, extra], axis=2).swapaxes(0, 1)
    pair = exchanged(tiles, "rep").sum(axis=0)
    width = sum(widths)
    sums, square = pair[:, :width], pair[:, width:]
    if kind != jnp.float32:
        lead = square.astype(kind)
        rest = (square - lead.astype(jnp.float32)).astype(kind)
        square = jnp.concatenate([lead, rest], axis=1)
        sums = sums.astype(kind)
    sent = jnp.concatenate([sums, square], axis=1)
    got = exchanged(sent[:, None, :], "seq")[:, 0].astype(jnp.float32).sum(axis=0)
    found, at = [], 0
    for w in widths:
        found.append(got[at : at + w])
        at += w
    total = got[at] if kind == jnp.float32 else got[at] + got[at + LANES]
    return found, total


def partial_attention(queries, key_rows, value_rows, usable):
    factor = 1.0 / math.sqrt(queries.shape[-1])
    scores = (
        jnp.einsum("ngd,tnd->ngt", queries, key_rows, preferred_element_type=jnp.float32) * factor
    )
    scores = jnp.where(usable[None, None, :], scores, FLOOR_SCORE)
    highest = jnp.max(scores, axis=-1)
    weights = jnp.where(usable[None, None, :], jnp.exp(scores - highest[..., None]), 0.0)
    totals = jnp.sum(weights, axis=-1)
    summed = jnp.einsum(
        "ngt,tnd->ngd",
        weights.astype(jnp.bfloat16),
        value_rows,
        preferred_element_type=jnp.float32,
    )
    return (highest, totals, summed)


def shards(
    tokens,
    attn_gain,
    ffn_gain,
    w_query,
    w_key,
    w_value,
    w_out,
    w_gate,
    w_up,
    w_down,
    kv_pool,
    lengths,
    pool_row,
    block_table,
):
    seq_count = tokens.shape[0]
    per_group = H // KVH
    slot_count = kv_pool.shape[2]
    half_rows = kv_pool.shape[3]
    row_here = lax.axis_index("seq")
    head_here = lax.axis_index("head")
    rep_here = lax.axis_index("rep")
    seq_ids = jnp.arange(seq_count, dtype=jnp.int32)
    to_row = pool_row[None, :] == seq_ids[:, None]
    owner_seq = jnp.sum(jnp.where(pool_row == row_here, seq_ids, 0))
    table_row = lax.dynamic_index_in_dim(block_table, owner_seq, 0, keepdims=False)
    length_here = lax.dynamic_index_in_dim(lengths, owner_seq, 0, keepdims=False)

    pool_local = kv_pool[:, 0]
    moved = []
    for side in range(2):
        by_head = lax.all_to_all(pool_local[side], "head", split_axis=2, concat_axis=0, tiled=True)
        logical = jnp.take(by_head, table_row, axis=0)
        moved.append(lax.all_to_all(logical, "seq", split_axis=0, concat_axis=0, tiled=True))
    here = row_here * BLK + rep_here * half_rows + jnp.arange(half_rows, dtype=jnp.int32)
    live_out = here[None, :] < lengths[:, None]
    decoded = jnp.stack(
        [
            jnp.where(live_out[:, :, None], jnp.take(m, pool_row, axis=0), jnp.zeros((), m.dtype))
            for m in moved
        ]
    )

    ordered = jnp.dot(
        to_row.astype(jnp.bfloat16), tokens, preferred_element_type=jnp.float32
    )
    residual = ordered
    squares = jnp.sum(residual * residual, axis=1)
    scaled = (residual * attn_gain).astype(jnp.bfloat16)
    (query, key_new, value_new), square_sum = rows_to_owner(
        [
            jnp.dot(scaled, w, preferred_element_type=jnp.float32).reshape(seq_count, 2, -1)
            for w in (w_query, w_key, w_value)
        ],
        squares,
        jnp.float32,
    )
    scale = lax.rsqrt(square_sum / D + EPSILON)
    position = length_here.astype(jnp.float32)
    query = rotate((query * scale).reshape(per_group, HD), position).astype(jnp.bfloat16)
    key_new = rotate((key_new * scale).reshape(1, HD), position).astype(jnp.bfloat16)
    value_new = (value_new * scale).reshape(1, HD).astype(jnp.bfloat16)
    every_query = from_everyone(query, ("head", "rep"))

    block_ids = jnp.arange(table_row.shape[0], dtype=jnp.int32)
    slot_ids = head_here * slot_count + jnp.arange(slot_count, dtype=jnp.int32)
    block_of_slot = jnp.sum(
        jnp.where(table_row[None, :] == slot_ids[:, None], block_ids[None, :], 0), axis=1
    )
    token_pos = (
        block_of_slot[:, None] * BLK
        + rep_here * half_rows
        + jnp.arange(half_rows, dtype=jnp.int32)[None, :]
    )
    usable = (token_pos < length_here).reshape(-1)
    highest, totals, summed = partial_attention(
        every_query,
        pool_local[0].reshape(-1, KVH, HD),
        pool_local[1].reshape(-1, KVH, HD),
        usable,
    )
    state = jnp.concatenate(
        [
            summed,
            jnp.broadcast_to(highest[..., None], summed.shape),
            jnp.broadcast_to(totals[..., None], summed.shape),
        ],
        axis=-1,
    )
    parts = exchanged(state, ("head", "rep"))
    tops, masses = parts[..., HD], parts[..., 2 * HD]
    factor = 1.0 / math.sqrt(HD)
    own_score = (
        jnp.sum(query.astype(jnp.float32) * key_new.astype(jnp.float32), axis=-1) * factor
    )
    largest = jnp.maximum(jnp.max(tops, axis=0), own_score)
    kept = jnp.exp(tops - largest[None])
    own = jnp.exp(own_score - largest)
    mass = jnp.sum(masses * kept, axis=0) + own
    mixed = (
        jnp.sum(parts[..., :HD] * kept[..., None], axis=0)
        + own[:, None] * value_new.astype(jnp.float32)
    ) / mass[:, None]
    attn = mixed.reshape(-1).astype(jnp.bfloat16)
    attn_half = from_everyone(attn, "seq")
    attn_rows = from_everyone(attn_half, "rep").swapaxes(0, 1).reshape(seq_count, -1)
    attn_proj = from_everyone(
        jnp.dot(attn_rows, w_out, preferred_element_type=jnp.float32), "head"
    ).sum(axis=0)
    middle = residual + attn_proj

    square_mid = jnp.sum(middle * middle, axis=1)
    scaled_mid = (middle * ffn_gain).astype(jnp.bfloat16)
    (gate, up), square_sum_mid = rows_to_owner(
        [
            jnp.dot(scaled_mid, w, preferred_element_type=jnp.float32).reshape(seq_count, 2, -1)
            for w in (w_gate, w_up)
        ],
        square_mid,
        jnp.bfloat16,
    )
    scale_mid = lax.rsqrt(square_sum_mid / D + EPSILON)
    hidden = (jax.nn.silu(gate * scale_mid) * (up * scale_mid)).astype(jnp.bfloat16)
    hidden_half = from_everyone(hidden, "seq")
    hidden_rows = from_everyone(hidden_half, "rep").swapaxes(0, 1).reshape(seq_count, -1)
    down_part = from_everyone(
        jnp.dot(hidden_rows, w_down, preferred_element_type=jnp.float32), "head"
    ).sum(axis=0)
    layer = (middle + down_part).astype(jnp.bfloat16)
    layer_out = jnp.dot(
        to_row.T.astype(jnp.bfloat16), layer, preferred_element_type=jnp.float32
    ).astype(jnp.bfloat16)
    return (layer_out, decoded)


def solution(mesh):
    in_specs = (
        P("groups", ("seq", "rep")),
        P(("seq", "rep")),
        P(("seq", "rep")),
        P(("seq", "rep"), "head"),
        P(("seq", "rep"), "head"),
        P(("seq", "rep"), "head"),
        P("head", ("seq", "rep")),
        P(("seq", "rep"), "head"),
        P(("seq", "rep"), "head"),
        P("head", ("seq", "rep")),
        P(None, ("groups", "seq"), "head", "rep", None),
        P("groups"),
        P("groups"),
        P("groups", None),
    )
    out_specs = (P("groups", ("seq", "rep")), P(None, "groups", ("seq", "rep"), "head"))
    return jax.shard_map(shards, mesh=mesh, in_specs=in_specs, out_specs=out_specs, check_vma=False)
```

```python
import functools
import math

import jax
import jax.numpy as jnp
from jax import lax
from jax.experimental import pallas as pl
from jax.experimental.pallas import tpu as pltpu
from jax.sharding import PartitionSpec as P

D = 4096
H = 32
KVH = 8
HD = 128
BLK = 128

EPSILON = 1e-05
ROPE_LOG = math.log(500000.0)
FLOOR_SCORE = -1e30
MESH = pl.DeviceIdType.MESH
BF16 = jnp.bfloat16
F32 = jnp.float32


def send(src, dst, send_sem, recv_sem, **where):
    pltpu.make_async_remote_copy(
        src_ref=src,
        dst_ref=dst,
        send_sem=send_sem,
        recv_sem=recv_sem,
        device_id=where,
        device_id_type=MESH,
    ).start()


def drain(ref, sem):
    pltpu.make_async_copy(ref, ref, sem).wait()


def dot(a, b):
    return jnp.dot(a, b, preferred_element_type=F32)


def both_parts(value):
    lead = value.astype(BF16)
    rest = (value - lead.astype(F32)).astype(BF16)
    return jnp.concatenate([lead, rest], axis=0)


def folded(product):
    rows = product.shape[0] // 2
    return product[:rows] + product[rows:]


def kernel(
    n_seq, n_head, n_rep,
    tok, again, fgain, wq, wk, wv, wo, wg, wu, wd, kv, use, turn, table, prow, lens,
    layer_out, decoded,
    xk, xv, zk, zv, rk, rv,
    own1, far1, got1, row1, tile3, state4, got4, swap5, got5, ag5, wide,
    part6, own7, far7, got7, out8, row8, ag9, pair9, part11,
    s_send, s_recv,
):
    z = lax.axis_index("seq")
    h = lax.axis_index("head")
    r = lax.axis_index("rep")
    other = 1 - r
    j = h * n_rep + r
    n_kv = n_head * n_rep
    rows = n_seq
    slots = kv.shape[1]
    half = kv.shape[2]
    width = xk.shape[2]

    barrier = pltpu.get_barrier_semaphore()

    def greet_seq(d, _):
        pl.semaphore_signal(
            barrier, inc=1, device_id={"seq": lax.rem(z + d, n_seq)}, device_id_type=MESH
        )
        return 0

    lax.fori_loop(1, n_seq, greet_seq, 0)
    for t in range(1, n_kv):
        peer = lax.rem(j + t, n_kv)
        pl.semaphore_signal(
            barrier,
            inc=1,
            device_id={"head": peer // n_rep, "rep": peer % n_rep},
            device_id_type=MESH,
        )

    x = tok[...]
    square = jnp.broadcast_to(jnp.sum(x * x, axis=1, keepdims=True), (rows, HD))
    y = both_parts(x * again[...])
    pq, pk, pv = (folded(dot(y, w[...])) for w in (wq, wk, wv))
    qn = pq.shape[1] // n_rep // HD
    for side, buf in ((0, own1), (1, far1)):
        mine = (r == 0) if side == 0 else (r != 0)
        for c in range(qn):
            buf[:, c, :] = jnp.where(
                mine, pq[:, c * HD : (c + 1) * HD], pq[:, (qn + c) * HD : (qn + c + 1) * HD]
            )
        buf[:, qn, :] = jnp.where(mine, pk[:, :HD], pk[:, HD:])
        buf[:, qn + 1, :] = jnp.where(mine, pv[:, :HD], pv[:, HD:])
        buf[:, qn + 2, :] = square
        buf[:, qn + 3, :] = jnp.zeros((rows, HD), F32)

    pl.semaphore_wait(barrier, n_seq - 1 + n_kv - 1)

    send(far1, got1, s_send.at[0], s_recv.at[0], rep=other)

    for c, box in ((0, xk), (1, xv)):
        for t in range(1, n_head):
            peer = lax.rem(h + t, n_head)
            send(
                kv.at[c, :, :, pl.ds(pl.multiple_of(peer * width, width), width)],
                box.at[pl.ds(h * slots, slots)],
                s_send.at[1 + c],
                s_recv.at[1 + c],
                head=peer,
            )
        box[pl.ds(h * slots, slots)] = kv[
            c, :, :, pl.ds(pl.multiple_of(h * width, width), width)
        ]

    drain(got1, s_recv.at[0])
    own1[...] = own1[...] + got1[...]

    def send_seq(src_of, dst, which, lo, hi):
        def body(d, _):
            peer = lax.rem(z + d, n_seq)
            send(src_of(peer), dst.at[z], s_send.at[which], s_recv.at[which], seq=peer)
            back = lax.rem(z + n_seq - d, n_seq)

            @pl.when(d * 2 != n_seq)
            def _():
                send(src_of(back), dst.at[z], s_send.at[which], s_recv.at[which], seq=back)

            return 0

        lax.fori_loop(lo, hi, body, 0)

    reach = n_seq // 2 + 1

    def all_rows(ref):
        return ref.at[pl.ds(0, n_seq - 1)]

    send_seq(lambda p: own1.at[p], row1, 3, 1, reach)
    row1[z] = own1[z]

    drain(all_rows(row1), s_recv.at[3])
    total = jnp.sum(row1[...], axis=0)
    scale = lax.rsqrt(total[qn + 2 : qn + 3, 0:1] / D + EPSILON)
    total = total * scale
    line = lax.broadcasted_iota(jnp.int32, (8, HD), 0)
    turned = total * turn[0:1, :] + pltpu.roll(total, HD // 2, 1) * turn[1:2, :]
    mine = jnp.where(line <= qn, turned, jnp.where(line == qn + 1, total, 0.0))
    mine = mine.astype(BF16).astype(F32)
    tile3[j] = mine
    for t in range(1, n_kv):
        peer = lax.rem(j + t, n_kv)
        send(
            tile3.at[j], tile3.at[j], s_send.at[4], s_recv.at[4],
            head=peer // n_rep, rep=peer % n_rep,
        )
    drain(tile3.at[pl.ds(0, n_kv - 1)], s_recv.at[4])

    factor = 1.0 / math.sqrt(HD)
    live = use[...] > 0.5
    lane = lax.broadcasted_iota(jnp.int32, (8, HD), 1)
    for g in range(n_kv):
        keys = kv[0, :, :, g * HD : (g + 1) * HD].reshape(slots * half, HD)
        values = kv[1, :, :, g * HD : (g + 1) * HD].reshape(slots * half, HD)
        scores = (
            lax.dot_general(
                tile3[g].astype(BF16), keys, (((1,), (1,)), ((), ())), preferred_element_type=F32
            )
            * factor
        )
        scores = jnp.where(live, scores, FLOOR_SCORE)
        top = jnp.max(scores, axis=1, keepdims=True)
        weights = jnp.where(live, jnp.exp(scores - top), 0.0)
        mass = jnp.sum(weights, axis=1, keepdims=True)
        state4[g, 0:8, :] = dot(weights.astype(BF16), values)
        state4[g, 8:16, :] = jnp.where(lane < HD // 2, top, mass)
    for t in range(1, n_kv):
        peer = lax.rem(j + t, n_kv)
        send(
            state4.at[peer], got4.at[j], s_send.at[5], s_recv.at[5],
            head=peer // n_rep, rep=peer % n_rep,
        )
    got4[j] = state4[j]
    drain(got4.at[pl.ds(0, n_kv - 1)], s_recv.at[5])
    own_score = jnp.sum(mine * mine[qn : qn + 1, :], axis=1, keepdims=True) * factor
    top = own_score
    for s in range(n_kv):
        top = jnp.maximum(top, got4[s, 8:16, 0:1])
    own = jnp.exp(own_score - top)
    mass = own
    mixed = own * mine[qn + 1 : qn + 2, :]
    for s in range(n_kv):
        kept = jnp.exp(got4[s, 8:16, 0:1] - top)
        mass = mass + kept * got4[s, 8:16, HD // 2 : HD // 2 + 1]
        mixed = mixed + kept * got4[s, 0:8, :]
    swap5[...] = mixed / mass
    send(swap5, got5, s_send.at[6], s_recv.at[6], rep=other)

    drain(xk.at[pl.ds(0, (n_head - 1) * slots)], s_recv.at[1])

    def order_keys(b, _):
        zk[b] = xk[table[b]]
        return 0

    lax.fori_loop(0, n_seq, order_keys, 0)

    drain(got5, s_recv.at[6])
    first = jnp.where(r == 0, swap5[...], got5[...])
    second = jnp.where(r == 0, got5[...], swap5[...])
    ag5[z] = jnp.where(line < qn, first, pltpu.roll(second, qn, 0)).astype(BF16)
    send_seq(lambda p: ag5.at[z], ag5, 7, 1, reach)
    send_seq(lambda p: zk.at[p], rk, 8, 1, reach)
    rk[z] = zk[z]

    drain(xv.at[pl.ds(0, (n_head - 1) * slots)], s_recv.at[2])

    def order_values(b, _):
        zv[b] = xv[table[b]]
        return 0

    lax.fori_loop(0, n_seq, order_values, 0)

    drain(all_rows(ag5), s_recv.at[7])
    wide[...] = ag5[...].astype(F32)
    acc = dot(wide[:, 0, :].astype(BF16), wo[0:HD, :])
    for g in range(1, n_rep * qn):
        acc = acc + dot(wide[:, g, :].astype(BF16), wo[g * HD : (g + 1) * HD, :])
    pad = jnp.zeros((rows, HD - acc.shape[1]), F32)
    part6[h] = jnp.concatenate([acc, pad], axis=1)
    for t in range(1, n_head):
        peer = lax.rem(h + t, n_head)
        send(part6.at[h], part6.at[h], s_send.at[9], s_recv.at[9], head=peer)
    drain(part6.at[pl.ds(0, n_head - 1)], s_recv.at[9])
    proj = part6[0]
    for s in range(1, n_head):
        proj = proj + part6[s]
    middle = x + proj[:, : x.shape[1]]

    square = jnp.broadcast_to(jnp.sum(middle * middle, axis=1, keepdims=True), (rows, HD))
    y = both_parts(middle * fgain[...])
    fn = wg.shape[1] // n_rep // HD
    for w, at in ((wg, 0), (wu, 8)):
        p = folded(dot(y, w[...]))
        for side, buf in ((0, own7), (1, far7)):
            here = (r == 0) if side == 0 else (r != 0)
            for c in range(fn):
                buf[:, at + c, :] = jnp.where(
                    here, p[:, c * HD : (c + 1) * HD], p[:, (fn + c) * HD : (fn + c + 1) * HD]
                )
            for c in range(fn, 8):
                buf[:, at + c, :] = square
    send(far7, got7, s_send.at[10], s_recv.at[10], rep=other)
    drain(got7, s_recv.at[10])
    own7[...] = own7[...] + got7[...]
    square = own7[:, 7, :]
    own7[:, 15, :] = square - square.astype(BF16).astype(F32)
    out8[...] = own7[...].astype(BF16)
    send_seq(lambda p: out8.at[p], row8, 11, 1, reach)
    row8[z] = out8[z]

    cut = reach - n_seq // 8
    send_seq(lambda p: zv.at[p], rv, 12, cut, reach)

    drain(all_rows(row8), s_recv.at[11])
    total = jnp.sum(row8[...].astype(F32), axis=0)
    scale = lax.rsqrt((total[7:8, 0:1] + total[15:16, 0:1]) / D + EPSILON)
    gate = total[0:8] * scale
    up = total[8:16] * scale
    hidden = gate / (1.0 + jnp.exp(-gate)) * up
    ag9[z] = jnp.where(line < fn, hidden, 0.0).astype(BF16)
    send_seq(lambda p: ag9.at[z], ag9, 13, 1, reach)
    send_seq(lambda p: zv.at[p], rv, 12, 1, cut)
    rv[z] = zv[z]

    drain(all_rows(ag9), s_recv.at[13])
    send(ag9, pair9, s_send.at[14], s_recv.at[14], rep=other)

    def down(ref, which):
        wide[...] = ref[...].astype(F32)
        acc = jnp.zeros((rows, x.shape[1]), F32)
        for c in range(fn):
            at = pl.multiple_of((which * fn + c) * HD, HD)
            acc = acc + dot(wide[:, c, :].astype(BF16), wd[pl.ds(at, HD), :])
        return acc

    acc = down(ag9, r)
    drain(pair9, s_recv.at[14])
    acc = acc + down(pair9, other)
    part11[h] = jnp.concatenate([acc, pad], axis=1)
    for t in range(1, n_head):
        peer = lax.rem(h + t, n_head)
        send(part11.at[h], part11.at[h], s_send.at[15], s_recv.at[15], head=peer)
    drain(part11.at[pl.ds(0, n_head - 1)], s_recv.at[15])
    proj = part11[0]
    for s in range(1, n_head):
        proj = proj + part11[s]
    layer_out[...] = middle + proj[:, : x.shape[1]]

    here = z * BLK + r * half + lax.broadcasted_iota(jnp.int32, (half, width), 0)
    for c, box, sem in ((0, rk, 8), (1, rv, 12)):
        drain(all_rows(box), s_recv.at[sem])

        def place(i, _):
            found = box[prow[i]]
            decoded[c, i] = jnp.where(here < lens[i], found, jnp.zeros((), found.dtype))
            return 0

        lax.fori_loop(0, rows, place, 0)

    drain(far1, s_send.at[0])
    for c, box in ((0, xk), (1, xv)):
        drain(box.at[pl.ds(0, (n_head - 1) * slots)], s_send.at[1 + c])
    drain(all_rows(own1), s_send.at[3])
    drain(tile3.at[pl.ds(0, n_kv - 1)], s_send.at[4])
    drain(state4.at[pl.ds(0, n_kv - 1)], s_send.at[5])
    drain(swap5, s_send.at[6])
    drain(all_rows(ag5), s_send.at[7])
    drain(all_rows(zk), s_send.at[8])
    drain(part6.at[pl.ds(0, n_head - 1)], s_send.at[9])
    drain(far7, s_send.at[10])
    drain(all_rows(out8), s_send.at[11])
    drain(all_rows(zv), s_send.at[12])
    drain(all_rows(ag9), s_send.at[13])
    drain(ag9, s_send.at[14])
    drain(part11.at[pl.ds(0, n_head - 1)], s_send.at[15])


def shards(
    tokens,
    attn_gain,
    ffn_gain,
    w_query,
    w_key,
    w_value,
    w_out,
    w_gate,
    w_up,
    w_down,
    kv_pool,
    lengths,
    pool_row,
    block_table,
):
    rows, features = tokens.shape
    n_seq, n_head, n_rep = (lax.axis_size(a) for a in ("seq", "head", "rep"))
    slots, half = kv_pool.shape[2:4]
    width = kv_pool.shape[4] // n_head
    row_here = lax.axis_index("seq")
    head_here = lax.axis_index("head")
    rep_here = lax.axis_index("rep")
    seq_ids = jnp.arange(rows, dtype=jnp.int32)
    to_row = pool_row[None, :] == seq_ids[:, None]
    owner = pool_row == row_here
    table_row = jnp.sum(jnp.where(owner[:, None], block_table, 0), axis=0)
    length_here = jnp.sum(jnp.where(owner, lengths, 0))

    residual = jnp.dot(to_row.astype(BF16), tokens, preferred_element_type=F32)
    block_ids = jnp.arange(table_row.shape[0], dtype=jnp.int32)
    slot_ids = head_here * slots + jnp.arange(slots, dtype=jnp.int32)
    block_of_slot = jnp.sum(
        jnp.where(table_row[None, :] == slot_ids[:, None], block_ids[None, :], 0), axis=1
    )
    token_pos = (
        block_of_slot[:, None] * BLK
        + rep_here * half
        + jnp.arange(half, dtype=jnp.int32)[None, :]
    )
    usable = (token_pos < length_here).astype(F32).reshape(1, slots * half)
    freq_table = jnp.exp(jnp.arange(HD // 2, dtype=F32) * (-2.0 * ROPE_LOG / HD))
    angles = length_here.astype(F32) * freq_table
    sine = jnp.sin(angles)
    cosine = jnp.cos(angles)
    turn = jnp.stack(
        [jnp.concatenate([cosine, cosine]), jnp.concatenate([-sine, sine])]
    )

    vmem = pl.BlockSpec(memory_space=pltpu.VMEM)
    smem = pl.BlockSpec(memory_space=pltpu.SMEM)
    ring = (n_seq, half, width)
    n_kv = n_head * n_rep
    layer, decoded = pl.pallas_call(
        functools.partial(kernel, n_seq, n_head, n_rep),
        out_shape=(
            jax.ShapeDtypeStruct((rows, features), F32),
            jax.ShapeDtypeStruct((2, rows, half, width), BF16),
        ),
        in_specs=[vmem] * 13 + [smem] * 3,
        out_specs=(vmem, vmem),
        scratch_shapes=[
            pltpu.VMEM((n_head * slots, half, width), BF16),
            pltpu.VMEM((n_head * slots, half, width), BF16),
            pltpu.VMEM(ring, BF16),
            pltpu.VMEM(ring, BF16),
            pltpu.VMEM(ring, BF16),
            pltpu.VMEM(ring, BF16),
            pltpu.VMEM((rows, 8, HD), F32),
            pltpu.VMEM((rows, 8, HD), F32),
            pltpu.VMEM((rows, 8, HD), F32),
            pltpu.VMEM((rows, 8, HD), F32),
            pltpu.VMEM((n_kv, 8, HD), F32),
            pltpu.VMEM((n_kv, 16, HD), F32),
            pltpu.VMEM((n_kv, 16, HD), F32),
            pltpu.VMEM((8, HD), F32),
            pltpu.VMEM((8, HD), F32),
            pltpu.VMEM((rows, 8, HD), BF16),
            pltpu.VMEM((rows, 8, HD), F32),
            pltpu.VMEM((n_head, rows, HD), F32),
            pltpu.VMEM((rows, 16, HD), F32),
            pltpu.VMEM((rows, 16, HD), F32),
            pltpu.VMEM((rows, 16, HD), F32),
            pltpu.VMEM((rows, 16, HD), BF16),
            pltpu.VMEM((rows, 16, HD), BF16),
            pltpu.VMEM((rows, 8, HD), BF16),
            pltpu.VMEM((rows, 8, HD), BF16),
            pltpu.VMEM((n_head, rows, HD), F32),
            pltpu.SemaphoreType.DMA((16,)),
            pltpu.SemaphoreType.DMA((16,)),
        ],
        compiler_params=pltpu.CompilerParams(
            collective_id=0, has_side_effects=True, vmem_limit_bytes=48 * 1024 * 1024
        ),
        name="decode_layer",
    )(
        residual,
        attn_gain[None, :],
        ffn_gain[None, :],
        w_query,
        w_key,
        w_value,
        w_out,
        w_gate,
        w_up,
        w_down,
        kv_pool[:, 0],
        usable,
        turn,
        table_row,
        pool_row,
        lengths,
    )
    layer_out = jnp.dot(
        to_row.T.astype(BF16), layer.astype(BF16), preferred_element_type=F32
    ).astype(BF16)
    return (layer_out, decoded)


def solution(mesh):
    in_specs = (
        P("groups", ("seq", "rep")),
        P(("seq", "rep")),
        P(("seq", "rep")),
        P(("seq", "rep"), "head"),
        P(("seq", "rep"), "head"),
        P(("seq", "rep"), "head"),
        P("head", ("seq", "rep")),
        P(("seq", "rep"), "head"),
        P(("seq", "rep"), "head"),
        P("head", ("seq", "rep")),
        P(None, ("groups", "seq"), "head", "rep", None),
        P("groups"),
        P("groups"),
        P("groups", None),
    )
    out_specs = (P("groups", ("seq", "rep")), P(None, "groups", ("seq", "rep"), "head"))
    return jax.shard_map(shards, mesh=mesh, in_specs=in_specs, out_specs=out_specs, check_vma=False)
```

```python
import functools
import math

import jax
import jax.numpy as jnp
from jax import lax
from jax.experimental import pallas as pl
from jax.experimental.pallas import tpu as pltpu
from jax.sharding import PartitionSpec as P

D = 4096
H = 32
KVH = 8
HD = 128
BLK = 128

EPSILON = 1e-05
ROPE_LOG = math.log(500000.0)
FLOOR_SCORE = -1e30
MESH = pl.DeviceIdType.MESH
BF16 = jnp.bfloat16
F32 = jnp.float32


def send(src, dst, send_sem, recv_sem, **where):
    pltpu.make_async_remote_copy(
        src_ref=src,
        dst_ref=dst,
        send_sem=send_sem,
        recv_sem=recv_sem,
        device_id=where,
        device_id_type=MESH,
    ).start()


def drain(ref, sem):
    pltpu.make_async_copy(ref, ref, sem).wait()


def dot(a, b):
    return jnp.dot(a, b, preferred_element_type=F32)


def across(a, b):
    return lax.dot_general(a, b, (((1,), (1,)), ((), ())), preferred_element_type=F32)


def both_parts(value):
    lead = value.astype(BF16)
    rest = (value - lead.astype(F32)).astype(BF16)
    return jnp.concatenate([lead, rest], axis=0)


def folded(product):
    rows = product.shape[0] // 2
    return product[:rows] + product[rows:]


def kernel(n_seq, n_head, n_rep, near, pieces, *refs):
    (
        tok_h, pvec_h, again_h, fgain_h, turn_h, wq_h, wk_h, wv_h, kv_h, wo_h, wg_h, wu_h, wd_h,
        table, prow, lens,
        layer_out, decoded,
        tok, pvec, again, fgain, turn, wq, wk, wv, kv, wo, wg, wu, wd,
    ) = refs[:31]
    count = 2 * pieces
    pool, ordered, arrived = (refs[31 + k * count : 31 + (k + 1) * count] for k in range(3))
    (
        own1, far1, got1, near1, part1, row1, tile3, state4, got4, swap5, got5, ag5, wide,
        part6, own7, far7, got7, near8, part8, row8, ag9, pair9, part11,
        s_send, s_recv, s_load, b_xsend, b_xrecv, b_send, b_recv,
    ) = refs[31 + 3 * count :]
    z = lax.axis_index("seq")
    h = lax.axis_index("head")
    r = lax.axis_index("rep")
    other = 1 - r
    j = h * n_rep + r
    n_kv = n_head * n_rep
    rows = n_seq
    blocks = n_seq // near
    k_here, g_here = z % near, z // near
    slots = kv.shape[1]
    half = kv.shape[2]
    held = slots * half
    some = half // pieces
    width = decoded.shape[3]

    loads = [
        pltpu.make_async_copy(src, dst, s_load.at[k])
        for k, (src, dst) in enumerate(
            zip(
                (kv_h.at[:, 0], tok_h, pvec_h, again_h, fgain_h, turn_h, wq_h, wk_h, wv_h,
                 wo_h, wg_h, wu_h, wd_h),
                (kv, tok, pvec, again, fgain, turn, wq, wk, wv, wo, wg, wu, wd),
            )
        )
    ]
    for load in loads:
        load.start()

    barrier = pltpu.get_barrier_semaphore()

    def greet_seq(d, _):
        pl.semaphore_signal(
            barrier, inc=1, device_id={"seq": lax.rem(z + d, n_seq)}, device_id_type=MESH
        )
        return 0

    lax.fori_loop(1, n_seq, greet_seq, 0)
    for t in range(1, n_kv):
        peer = lax.rem(j + t, n_kv)
        pl.semaphore_signal(
            barrier,
            inc=1,
            device_id={"head": peer // n_rep, "rep": peer % n_rep},
            device_id_type=MESH,
        )
    loads[0].wait()
    pl.semaphore_wait(barrier, n_seq - 1 + n_kv - 1)

    def columns(q, owner):
        return (
            q // pieces,
            slice(None),
            pl.ds((q % pieces) * some, some),
            pl.ds(pl.multiple_of(owner * width, width), width),
        )

    for q in range(count):
        for t in range(1, n_head):
            peer = lax.rem(h + t, n_head)
            send(
                kv.at[columns(q, peer)],
                pool[q].at[pl.ds(h * slots, slots)],
                b_xsend.at[q],
                b_xrecv.at[q],
                head=peer,
            )

    for load in loads[1:9]:
        load.wait()
    at = lax.broadcasted_iota(jnp.int32, (rows, rows), 0)
    to_row = (at % blocks) * near + at // blocks == pvec[...]
    to_row = to_row.astype(F32).astype(BF16)
    x = dot(to_row, tok[...])
    square = jnp.broadcast_to(jnp.sum(x * x, axis=1, keepdims=True), (rows, HD))
    y = both_parts(x * again[...])
    pq, pk, pv = (folded(dot(y, w[...])) for w in (wq, wk, wv))
    qn = pq.shape[1] // n_rep // HD
    for side, buf in ((1, far1), (0, own1)):
        mine = (r == 0) if side == 0 else (r != 0)
        for c in range(qn):
            buf[:, c, :] = jnp.where(
                mine, pq[:, c * HD : (c + 1) * HD], pq[:, (qn + c) * HD : (qn + c + 1) * HD]
            )
        buf[:, qn, :] = jnp.where(mine, pk[:, :HD], pk[:, HD:])
        buf[:, qn + 1, :] = jnp.where(mine, pv[:, :HD], pv[:, HD:])
        buf[:, qn + 2, :] = square
        buf[:, qn + 3, :] = jnp.zeros((rows, HD), F32)
        if side == 1:
            send(far1, got1, s_send.at[0], s_recv.at[0], rep=other)

    def mates(part_of, dst, which):
        for t in range(1, near):
            peer = lax.rem(k_here + t, near)
            send(
                part_of(peer), dst, s_send.at[which], s_recv.at[which], seq=g_here * near + peer
            )

    def across_runs(part_of, dst, which):
        for t in range(1, blocks):
            peer = lax.rem(g_here + t, blocks)
            send(
                part_of(peer), dst, s_send.at[which], s_recv.at[which], seq=peer * near + k_here
            )

    def of_class(ref, k):
        return ref.at[pl.ds(k * blocks, blocks)]

    drain(got1, s_recv.at[0])
    own1[...] = own1[...] + got1[...]
    mates(lambda k: of_class(own1, k), near1.at[k_here], 1)
    near1[k_here] = own1[pl.ds(k_here * blocks, blocks)]
    drain(near1.at[pl.ds(0, near - 1)], s_recv.at[1])
    part1[...] = jnp.sum(near1[...], axis=0)
    across_runs(lambda g: part1.at[g], row1.at[g_here], 2)
    row1[g_here] = part1[g_here]

    owner = lax.fori_loop(0, rows, lambda i, at: jnp.where(prow[i] == z, i, at), 0)
    length = lens[owner]

    def put_in_order(q):
        pool[q][pl.ds(h * slots, slots)] = kv[columns(q, h)]
        drain(pool[q].at[pl.ds(0, (n_head - 1) * slots)], b_xrecv.at[q])

        def one(b, _):
            ordered[q][b] = pool[q][table[owner, b]]
            return 0

        lax.fori_loop(0, n_seq, one, 0)
        arrived[q][z] = ordered[q][z]

    reach = n_seq // 2 + 1

    def bulk(q, lo, hi):
        def body(d, _):
            peer = lax.rem(z + d, n_seq)
            send(ordered[q].at[peer], arrived[q].at[z], b_send.at[q], b_recv.at[q], seq=peer)
            back = lax.rem(z + n_seq - d, n_seq)

            @pl.when(d * 2 != n_seq)
            def _():
                send(ordered[q].at[back], arrived[q].at[z], b_send.at[q], b_recv.at[q], seq=back)

            return 0

        lax.fori_loop(lo, hi, body, 0)

    cuts = (1, 1 + n_seq * 9 // 32, 1 + n_seq * 13 // 32, reach)

    put_in_order(0)
    bulk(0, 1, reach)

    slot_of = lax.broadcasted_iota(jnp.int32, (1, held), 1) // half
    place_of = lax.broadcasted_iota(jnp.int32, (1, held), 1) % half

    def note_block(b, at):
        return jnp.where(slot_of + h * slots == table[owner, b], b, at)

    block_of = lax.fori_loop(0, n_seq, note_block, jnp.zeros((1, held), jnp.int32))
    live = block_of * BLK + r * half + place_of < length

    drain(row1.at[pl.ds(0, blocks - 1)], s_recv.at[2])
    total = jnp.sum(row1[...], axis=0)
    scale = lax.rsqrt(total[qn + 2 : qn + 3, 0:1] / D + EPSILON)
    total = total * scale
    line = lax.broadcasted_iota(jnp.int32, (8, HD), 0)
    turned = total * turn[0:1, :] + pltpu.roll(total, HD // 2, 1) * turn[1:2, :]
    mine = jnp.where(line <= qn, turned, jnp.where(line == qn + 1, total, 0.0))
    mine = mine.astype(BF16).astype(F32)
    tile3[j] = mine
    for t in range(1, n_kv):
        peer = lax.rem(j + t, n_kv)
        send(
            tile3.at[j], tile3.at[j], s_send.at[3], s_recv.at[3],
            head=peer // n_rep, rep=peer % n_rep,
        )
    drain(tile3.at[pl.ds(0, n_kv - 1)], s_recv.at[3])

    factor = 1.0 / math.sqrt(HD)
    lane = lax.broadcasted_iota(jnp.int32, (8, HD), 1)
    for g in range(n_kv):
        keys = kv[0, :, :, g * HD : (g + 1) * HD].reshape(held, HD)
        values = kv[1, :, :, g * HD : (g + 1) * HD].reshape(held, HD)
        scores = across(tile3[g].astype(BF16), keys) * factor
        scores = jnp.where(live, scores, FLOOR_SCORE)
        top = jnp.max(scores, axis=1, keepdims=True)
        weights = jnp.where(live, jnp.exp(scores - top), 0.0)
        mass = jnp.sum(weights, axis=1, keepdims=True)
        state4[g, 0:8, :] = dot(weights.astype(BF16), values)
        state4[g, 8:16, :] = jnp.where(lane < HD // 2, top, mass)
    for t in range(1, n_kv):
        peer = lax.rem(j + t, n_kv)
        send(
            state4.at[peer], got4.at[j], s_send.at[4], s_recv.at[4],
            head=peer // n_rep, rep=peer % n_rep,
        )
    got4[j] = state4[j]
    put_in_order(1)
    drain(got4.at[pl.ds(0, n_kv - 1)], s_recv.at[4])
    own_score = jnp.sum(mine * mine[qn : qn + 1, :], axis=1, keepdims=True) * factor
    top = own_score
    for s in range(n_kv):
        top = jnp.maximum(top, got4[s, 8:16, 0:1])
    own = jnp.exp(own_score - top)
    mass = own
    mixed = own * mine[qn + 1 : qn + 2, :]
    for s in range(n_kv):
        kept = jnp.exp(got4[s, 8:16, 0:1] - top)
        mass = mass + kept * got4[s, 8:16, HD // 2 : HD // 2 + 1]
        mixed = mixed + kept * got4[s, 0:8, :]
    swap5[...] = mixed / mass
    send(swap5, got5, s_send.at[5], s_recv.at[5], rep=other)
    drain(got5, s_recv.at[5])
    first = jnp.where(r == 0, swap5[...], got5[...])
    second = jnp.where(r == 0, got5[...], swap5[...])
    slot_here = k_here * blocks + g_here
    ag5[slot_here] = jnp.where(line < qn, first, pltpu.roll(second, qn, 0)).astype(BF16)
    across_runs(lambda g: ag5.at[slot_here], ag5.at[slot_here], 6)
    bulk(1, cuts[2], cuts[3])
    drain(ag5.at[pl.ds(0, blocks - 1)], s_recv.at[6])
    mates(lambda k: of_class(ag5, k_here), of_class(ag5, k_here), 7)
    bulk(1, cuts[1], cuts[2])
    for load in loads[9:]:
        load.wait()
    put_in_order(2)
    drain(ag5.at[pl.ds(0, (near - 1) * blocks)], s_recv.at[7])

    wide[...] = ag5[...].astype(F32)
    acc = across(wide[:, 0, :].astype(BF16), wo[:, 0:HD])
    for g in range(1, n_rep * qn):
        acc = acc + across(wide[:, g, :].astype(BF16), wo[:, g * HD : (g + 1) * HD])
    pad = jnp.zeros((rows, HD - acc.shape[1]), F32)
    part6[h] = jnp.concatenate([acc, pad], axis=1)
    for t in range(1, n_head):
        peer = lax.rem(h + t, n_head)
        send(part6.at[h], part6.at[h], s_send.at[8], s_recv.at[8], head=peer)
    drain(part6.at[pl.ds(0, n_head - 1)], s_recv.at[8])
    proj = part6[0]
    for s in range(1, n_head):
        proj = proj + part6[s]
    middle = x + proj[:, : x.shape[1]]

    square = jnp.broadcast_to(jnp.sum(middle * middle, axis=1, keepdims=True), (rows, HD))
    y = both_parts(middle * fgain[...])
    fn = wg.shape[1] // n_rep // HD
    pg, pu = (folded(dot(y, w[...])) for w in (wg, wu))
    for side, buf in ((1, far7), (0, own7)):
        here = (r == 0) if side == 0 else (r != 0)
        for p, start in ((pg, 0), (pu, 8)):
            for c in range(fn):
                buf[:, start + c, :] = jnp.where(
                    here, p[:, c * HD : (c + 1) * HD], p[:, (fn + c) * HD : (fn + c + 1) * HD]
                )
            for c in range(fn, 8):
                buf[:, start + c, :] = square
        if side == 1:
            send(far7, got7, s_send.at[9], s_recv.at[9], rep=other)
    drain(got7, s_recv.at[9])
    own7[...] = own7[...] + got7[...]
    mates(lambda k: of_class(own7, k), near8.at[k_here], 10)
    near8[k_here] = own7[pl.ds(k_here * blocks, blocks)]
    bulk(1, cuts[0], cuts[1])
    drain(near8.at[pl.ds(0, near - 1)], s_recv.at[10])
    total = jnp.sum(near8[...], axis=0)
    square = total[:, 7, :]
    near8[0] = total
    near8[0, :, 15, :] = square - square.astype(BF16).astype(F32)
    part8[...] = near8[0].astype(BF16)
    across_runs(lambda g: part8.at[g], row8.at[g_here], 11)
    row8[g_here] = part8[g_here]
    bulk(2, cuts[2], cuts[3])
    put_in_order(3)

    drain(row8.at[pl.ds(0, blocks - 1)], s_recv.at[11])
    total = jnp.sum(row8[...].astype(F32), axis=0)
    scale = lax.rsqrt((total[7:8, 0:1] + total[15:16, 0:1]) / D + EPSILON)
    gate = total[0:8] * scale
    up = total[8:16] * scale
    hidden = gate / (1.0 + jnp.exp(-gate)) * up
    ag9[slot_here] = jnp.where(line < fn, hidden, 0.0).astype(BF16)
    across_runs(lambda g: ag9.at[slot_here], ag9.at[slot_here], 12)
    bulk(2, cuts[1], cuts[2])
    drain(ag9.at[pl.ds(0, blocks - 1)], s_recv.at[12])
    mates(lambda k: of_class(ag9, k_here), of_class(ag9, k_here), 13)
    bulk(2, cuts[0], cuts[1])
    bulk(3, 1, reach)
    drain(ag9.at[pl.ds(0, (near - 1) * blocks)], s_recv.at[13])
    send(ag9, pair9, s_send.at[14], s_recv.at[14], rep=other)

    def down(ref, which):
        wide[...] = ref[...].astype(F32)
        acc = jnp.zeros((rows, x.shape[1]), F32)
        for c in range(fn):
            start = pl.multiple_of((which * fn + c) * HD, HD)
            acc = acc + across(wide[:, c, :].astype(BF16), wd[:, pl.ds(start, HD)])
        return acc

    acc = down(ag9, r)
    drain(pair9, s_recv.at[14])
    acc = acc + down(pair9, other)
    part11[h] = jnp.concatenate([acc, pad], axis=1)
    for t in range(1, n_head):
        peer = lax.rem(h + t, n_head)
        send(part11.at[h], part11.at[h], s_send.at[15], s_recv.at[15], head=peer)
    drain(part11.at[pl.ds(0, n_head - 1)], s_recv.at[15])
    proj = part11[0]
    for s in range(1, n_head):
        proj = proj + part11[s]
    layer = (middle + proj[:, : x.shape[1]]).astype(BF16)
    layer_out[...] = lax.dot_general(
        to_row, layer, (((0,), (0,)), ((), ())), preferred_element_type=F32
    ).astype(BF16)

    for q in range(count):
        start = (q % pieces) * some
        here = z * BLK + r * half + start + lax.broadcasted_iota(jnp.int32, (some, width), 0)
        drain(arrived[q].at[pl.ds(0, n_seq - 1)], b_recv.at[q])

        def place(i, _):
            found = arrived[q][prow[i]]
            decoded[q // pieces, i, start : start + some, :] = jnp.where(
                here < lens[i], found, jnp.zeros((), found.dtype)
            )
            return 0

        lax.fori_loop(0, rows, place, 0)

    for q in range(count):
        drain(pool[q].at[pl.ds(0, (n_head - 1) * slots)], b_xsend.at[q])
        drain(ordered[q].at[pl.ds(0, n_seq - 1)], b_send.at[q])
    drain(far1, s_send.at[0])
    drain(near1.at[pl.ds(0, near - 1)], s_send.at[1])
    drain(row1.at[pl.ds(0, blocks - 1)], s_send.at[2])
    drain(tile3.at[pl.ds(0, n_kv - 1)], s_send.at[3])
    drain(state4.at[pl.ds(0, n_kv - 1)], s_send.at[4])
    drain(swap5, s_send.at[5])
    drain(ag5.at[pl.ds(0, blocks - 1)], s_send.at[6])
    drain(ag5.at[pl.ds(0, (near - 1) * blocks)], s_send.at[7])
    drain(part6.at[pl.ds(0, n_head - 1)], s_send.at[8])
    drain(far7, s_send.at[9])
    drain(near8.at[pl.ds(0, near - 1)], s_send.at[10])
    drain(row8.at[pl.ds(0, blocks - 1)], s_send.at[11])
    drain(ag9.at[pl.ds(0, blocks - 1)], s_send.at[12])
    drain(ag9.at[pl.ds(0, (near - 1) * blocks)], s_send.at[13])
    drain(ag9, s_send.at[14])
    drain(part11.at[pl.ds(0, n_head - 1)], s_send.at[15])


def shards(
    tokens,
    attn_gain,
    ffn_gain,
    w_query,
    w_key,
    w_value,
    w_out,
    w_gate,
    w_up,
    w_down,
    kv_pool,
    lengths,
    pool_row,
    block_table,
):
    rows, features = tokens.shape
    n_seq, n_head, n_rep = (lax.axis_size(a) for a in ("seq", "head", "rep"))
    slots, half = kv_pool.shape[2:4]
    width = kv_pool.shape[4] // n_head
    n_kv = n_head * n_rep

    position = jnp.sum(jnp.where(pool_row == lax.axis_index("seq"), lengths, 0)).astype(F32)
    freq_table = jnp.exp(jnp.arange(HD // 2, dtype=F32) * (-2.0 * ROPE_LOG / HD))
    angles = position * freq_table
    sine = jnp.sin(angles)
    cosine = jnp.cos(angles)
    turn = jnp.stack([jnp.concatenate([cosine, cosine]), jnp.concatenate([-sine, sine])])

    given = (
        tokens,
        pool_row[None, :],
        attn_gain[None, :],
        ffn_gain[None, :],
        turn,
        w_query,
        w_key,
        w_value,
        kv_pool,
        w_out.T,
        w_gate,
        w_up,
        w_down.T,
    )
    vmem = pl.BlockSpec(memory_space=pltpu.VMEM)
    smem = pl.BlockSpec(memory_space=pltpu.SMEM)
    pieces, near = 2, 4
    blocks = n_seq // near
    pool = (n_head * slots, half // pieces, width)
    ring = (n_seq, half // pieces, width)
    line, lines = (rows, 8, HD), (rows, 16, HD)
    return pl.pallas_call(
        functools.partial(kernel, n_seq, n_head, n_rep, near, pieces),
        out_shape=(
            jax.ShapeDtypeStruct((rows, features), BF16),
            jax.ShapeDtypeStruct((2, rows, half, width), BF16),
        ),
        in_specs=[pl.BlockSpec(memory_space=pl.ANY)] * len(given) + [smem] * 3,
        out_specs=(vmem, vmem),
        scratch_shapes=[
            *(pltpu.VMEM(a.shape, a.dtype) for a in given[:8]),
            pltpu.VMEM((2, *kv_pool.shape[2:]), BF16),
            *(pltpu.VMEM(a.shape, a.dtype) for a in given[9:]),
            *(pltpu.VMEM(pool, BF16) for _ in range(2 * pieces)),
            *(pltpu.VMEM(ring, BF16) for _ in range(4 * pieces)),
            *(pltpu.VMEM(line, F32) for _ in range(3)),
            pltpu.VMEM((near, blocks, 8, HD), F32),
            pltpu.VMEM((blocks, 8, HD), F32),
            pltpu.VMEM((blocks, 8, HD), F32),
            pltpu.VMEM((n_kv, 8, HD), F32),
            pltpu.VMEM((n_kv, 16, HD), F32),
            pltpu.VMEM((n_kv, 16, HD), F32),
            pltpu.VMEM((8, HD), F32),
            pltpu.VMEM((8, HD), F32),
            pltpu.VMEM(line, BF16),
            pltpu.VMEM(line, F32),
            pltpu.VMEM((n_head, rows, HD), F32),
            *(pltpu.VMEM(lines, F32) for _ in range(3)),
            pltpu.VMEM((near, blocks, 16, HD), F32),
            pltpu.VMEM((blocks, 16, HD), BF16),
            pltpu.VMEM((blocks, 16, HD), BF16),
            *(pltpu.VMEM(line, BF16) for _ in range(2)),
            pltpu.VMEM((n_head, rows, HD), F32),
            pltpu.SemaphoreType.DMA((16,)),
            pltpu.SemaphoreType.DMA((16,)),
            pltpu.SemaphoreType.DMA((len(given),)),
            *(pltpu.SemaphoreType.DMA((2 * pieces,)) for _ in range(4)),
        ],
        compiler_params=pltpu.CompilerParams(
            collective_id=0, has_side_effects=True, vmem_limit_bytes=60 * 1024 * 1024
        ),
        name="decode_layer",
    )(*given, block_table, pool_row, lengths)


def solution(mesh):
    in_specs = (
        P("groups", ("seq", "rep")),
        P(("seq", "rep")),
        P(("seq", "rep")),
        P(("seq", "rep"), "head"),
        P(("seq", "rep"), "head"),
        P(("seq", "rep"), "head"),
        P("head", ("seq", "rep")),
        P(("seq", "rep"), "head"),
        P(("seq", "rep"), "head"),
        P("head", ("seq", "rep")),
        P(None, ("groups", "seq"), "head", "rep", None),
        P("groups"),
        P("groups"),
        P("groups", None),
    )
    out_specs = (P("groups", ("seq", "rep")), P(None, "groups", ("seq", "rep"), "head"))
    return jax.shard_map(shards, mesh=mesh, in_specs=in_specs, out_specs=out_specs, check_vma=False)
```

```python
import functools
import math

import jax
import jax.numpy as jnp
import numpy as np
from jax import lax
from jax.experimental import pallas as pl
from jax.experimental.pallas import tpu as pltpu
from jax.sharding import PartitionSpec as P

D = 4096
H = 32
KVH = 8
HD = 128
BLK = 128

EPSILON = 1e-05
ROPE_LOG = math.log(500000.0)
FLOOR_SCORE = -1e30
STEP = 64
PIECES = 4
WAVES = ((0, 1), (2,), (3,), (4,), (5,), (6,), (7,))
MESH = pl.DeviceIdType.MESH
BF16 = jnp.bfloat16
F32 = jnp.float32


def send(src, dst, send_sem, recv_sem, **where):
    pltpu.make_async_remote_copy(
        src_ref=src,
        dst_ref=dst,
        send_sem=send_sem,
        recv_sem=recv_sem,
        device_id=where,
        device_id_type=MESH,
    ).start()


def drain(ref, sem):
    pltpu.make_async_copy(ref, ref, sem).wait()


def dot(a, b):
    return jnp.dot(a, b, preferred_element_type=F32)


def across(a, b):
    return lax.dot_general(a, b, (((1,), (1,)), ((), ())), preferred_element_type=F32)


def both_parts(value):
    lead = value.astype(BF16)
    rest = (value - lead.astype(F32)).astype(BF16)
    return jnp.concatenate([lead, rest], axis=0)


def folded(product):
    rows = product.shape[0] // 2
    return product[:rows] + product[rows:]


def kernel(n_seq, n_head, n_rep, near, pieces, *refs):
    (
        tok_h, pvec_h, again_h, fgain_h, far_h, fine_h, wq_h, wk_h, wv_h, kv_h, wo_h, wg_h, wu_h, wd_h,
        table_h, prow_h, lens_h,
        layer_out, decoded,
        tok, pvec, again, fgain, far, fine, wq, wk, wv, kv, wo, wg, wu, wd,
        table, prow, lens,
    ) = refs[:36]
    count = 2 * pieces
    pool, ordered, arrived = (refs[36 + k * count : 36 + (k + 1) * count] for k in range(3))
    (
        own1, far1, got1, near1, part1, row1, tile3, state4, got4, swap5, got5, ag5, wide,
        part6, own7, far7, got7, near8, part8, row8, ag9, pair9, part11,
        s_send, s_recv, s_load, b_xsend, b_xrecv, b_send, b_recv,
    ) = refs[36 + 3 * count :]
    z = lax.axis_index("seq")
    h = lax.axis_index("head")
    r = lax.axis_index("rep")
    other = 1 - r
    j = h * n_rep + r
    n_kv = n_head * n_rep
    rows = n_seq
    blocks = n_seq // near
    k_here, g_here = z % near, z // near
    slots = kv.shape[1]
    half = kv.shape[2]
    held = slots * half
    some = half // pieces
    width = decoded.shape[3]

    barrier = pltpu.get_barrier_semaphore()

    for d in range(1, n_seq):
        d = (n_seq - d + d % 2) // 2 * (1 if d % 2 else -1)
        pl.semaphore_signal(
            barrier, inc=1, device_id={"seq": lax.rem(z + d + n_seq, n_seq)}, device_id_type=MESH
        )
    for t in range(1, n_kv):
        peer = lax.rem(j + t, n_kv)
        pl.semaphore_signal(
            barrier,
            inc=1,
            device_id={"head": peer // n_rep, "rep": peer % n_rep},
            device_id_type=MESH,
        )
    loads = [
        pltpu.make_async_copy(src, dst, s_load.at[k])
        for k, (src, dst) in enumerate(
            zip(
                (kv_h.at[:, 0], tok_h, pvec_h, again_h, fgain_h, far_h, fine_h, wq_h, wk_h, wv_h,
                 table_h, prow_h, lens_h, wo_h, wg_h, wu_h, wd_h),
                (kv, tok, pvec, again, fgain, far, fine, wq, wk, wv,
                 table, prow, lens, wo, wg, wu, wd),
            )
        )
    ]
    for load in loads:
        load.start()

    loads[0].wait()
    pl.semaphore_wait(barrier, n_seq - 1 + n_kv - 1)

    def columns(q, owner):
        return (
            q // pieces,
            slice(None),
            pl.ds((q % pieces) * some, some),
            pl.ds(pl.multiple_of(owner * width, width), width),
        )

    for q in range(count):
        for t in range(1, n_head):
            peer = lax.rem(h + t, n_head)
            send(
                kv.at[columns(q, peer)],
                pool[q].at[pl.ds(h * slots, slots)],
                b_xsend.at[q],
                b_xrecv.at[q],
                head=peer,
            )

    for load in loads[1:13]:
        load.wait()
    at = lax.broadcasted_iota(jnp.int32, (rows, rows), 0)
    to_row = (at % blocks) * near + at // blocks == pvec[...]
    to_row = to_row.astype(F32).astype(BF16)
    x = dot(to_row, tok[...])
    square = jnp.broadcast_to(jnp.sum(x * x, axis=1, keepdims=True), (rows, HD))
    y = both_parts(x * again[...])
    pq, pk, pv = (folded(dot(y, w[...])) for w in (wq, wk, wv))
    qn = pq.shape[1] // n_rep // HD
    for side, buf in ((1, far1), (0, own1)):
        mine = (r == 0) if side == 0 else (r != 0)
        for c in range(qn):
            buf[:, c, :] = jnp.where(
                mine, pq[:, c * HD : (c + 1) * HD], pq[:, (qn + c) * HD : (qn + c + 1) * HD]
            )
        buf[:, qn, :] = jnp.where(mine, pk[:, :HD], pk[:, HD:])
        buf[:, qn + 1, :] = jnp.where(mine, pv[:, :HD], pv[:, HD:])
        buf[:, qn + 2, :] = square
        buf[:, qn + 3, :] = jnp.zeros((rows, HD), F32)
        if side == 1:
            send(far1, got1, s_send.at[0], s_recv.at[0], rep=other)

    def mates(part_of, dst, which):
        for t in range(1, near):
            peer = lax.rem(k_here + t, near)
            send(
                part_of(peer), dst, s_send.at[which], s_recv.at[which], seq=g_here * near + peer
            )

    def across_runs(part_of, dst, which):
        for t in range(1, blocks):
            peer = lax.rem(g_here + t, blocks)
            send(
                part_of(peer), dst, s_send.at[which], s_recv.at[which], seq=peer * near + k_here
            )

    def of_class(ref, k):
        return ref.at[pl.ds(k * blocks, blocks)]

    drain(got1, s_recv.at[0])
    own1[...] = own1[...] + got1[...]
    mates(lambda k: of_class(own1, k), near1.at[k_here], 1)
    near1[k_here] = own1[pl.ds(k_here * blocks, blocks)]
    drain(near1.at[pl.ds(0, near - 1)], s_recv.at[1])
    part1[...] = jnp.sum(near1[...], axis=0)
    across_runs(lambda g: part1.at[g], row1.at[g_here], 2)
    row1[g_here] = part1[g_here]

    owner = lax.fori_loop(0, rows, lambda i, at: jnp.where(prow[i] == z, i, at), 0)
    length = lens[owner]

    def put_in_order(q):
        pool[q][pl.ds(h * slots, slots)] = kv[columns(q, h)]
        drain(pool[q].at[pl.ds(0, (n_head - 1) * slots)], b_xrecv.at[q])

        def one(b, _):
            ordered[q][b] = pool[q][table[owner, b]]
            return 0

        lax.fori_loop(0, n_seq, one, 0)
        arrived[q][z] = ordered[q][z]

    reach = n_seq // 2 + 1

    def bulk(q, lo, hi):
        def body(d, _):
            peer = lax.rem(z + d, n_seq)
            send(ordered[q].at[peer], arrived[q].at[z], b_send.at[q], b_recv.at[q], seq=peer)
            back = lax.rem(z + n_seq - d, n_seq)

            @pl.when(d * 2 != n_seq)
            def _():
                send(ordered[q].at[back], arrived[q].at[z], b_send.at[q], b_recv.at[q], seq=back)

            return 0

        lax.fori_loop(lo, hi, body, 0)

    def wave(n):
        for q in WAVES[n]:
            put_in_order(q)
            bulk(q, 1, reach)

    wave(0)

    slot_of = lax.broadcasted_iota(jnp.int32, (1, held), 1) // half
    place_of = lax.broadcasted_iota(jnp.int32, (1, held), 1) % half

    def note_block(b, at):
        return jnp.where(slot_of + h * slots == table[owner, b], b, at)

    block_of = lax.fori_loop(0, n_seq, note_block, jnp.zeros((1, held), jnp.int32))
    live = block_of * BLK + r * half + place_of < length

    drain(row1.at[pl.ds(0, blocks - 1)], s_recv.at[2])
    total = jnp.sum(row1[...], axis=0)
    scale = lax.rsqrt(total[qn + 2 : qn + 3, 0:1] / D + EPSILON)
    total = total * scale
    line = lax.broadcasted_iota(jnp.int32, (8, HD), 0)
    lane = lax.broadcasted_iota(jnp.int32, (8, HD), 1)
    whole, part = far[length // STEP], fine[length % STEP]
    cosine = whole[0:1] * part[0:1] - whole[1:2] * part[1:2]
    sine = whole[1:2] * part[0:1] + whole[0:1] * part[1:2]
    sine = jnp.where(lane < HD // 2, -sine, sine)
    turned = total * cosine + pltpu.roll(total, HD // 2, 1) * sine
    mine = jnp.where(line <= qn, turned, jnp.where(line == qn + 1, total, 0.0))
    mine = mine.astype(BF16).astype(F32)
    tile3[j] = mine
    for t in range(1, n_kv):
        peer = lax.rem(j + t, n_kv)
        send(
            tile3.at[j], tile3.at[j], s_send.at[3], s_recv.at[3],
            head=peer // n_rep, rep=peer % n_rep,
        )
    drain(tile3.at[pl.ds(0, n_kv - 1)], s_recv.at[3])

    factor = 1.0 / math.sqrt(HD)
    for g in range(n_kv):
        keys = kv[0, :, :, g * HD : (g + 1) * HD].reshape(held, HD)
        values = kv[1, :, :, g * HD : (g + 1) * HD].reshape(held, HD)
        scores = across(tile3[g].astype(BF16), keys) * factor
        scores = jnp.where(live, scores, FLOOR_SCORE)
        top = jnp.max(scores, axis=1, keepdims=True)
        weights = jnp.where(live, jnp.exp(scores - top), 0.0)
        mass = jnp.sum(weights, axis=1, keepdims=True)
        state4[g, 0:8, :] = dot(weights.astype(BF16), values)
        state4[g, 8:16, :] = jnp.where(lane < HD // 2, top, mass)
    for t in range(1, n_kv):
        peer = lax.rem(j + t, n_kv)
        send(
            state4.at[peer], got4.at[j], s_send.at[4], s_recv.at[4],
            head=peer // n_rep, rep=peer % n_rep,
        )
    got4[j] = state4[j]
    drain(got4.at[pl.ds(0, n_kv - 1)], s_recv.at[4])
    own_score = jnp.sum(mine * mine[qn : qn + 1, :], axis=1, keepdims=True) * factor
    top = own_score
    for s in range(n_kv):
        top = jnp.maximum(top, got4[s, 8:16, 0:1])
    own = jnp.exp(own_score - top)
    mass = own
    mixed = own * mine[qn + 1 : qn + 2, :]
    for s in range(n_kv):
        kept = jnp.exp(got4[s, 8:16, 0:1] - top)
        mass = mass + kept * got4[s, 8:16, HD // 2 : HD // 2 + 1]
        mixed = mixed + kept * got4[s, 0:8, :]
    swap5[...] = mixed / mass
    send(swap5, got5, s_send.at[5], s_recv.at[5], rep=other)
    drain(got5, s_recv.at[5])
    first = jnp.where(r == 0, swap5[...], got5[...])
    second = jnp.where(r == 0, got5[...], swap5[...])
    slot_here = k_here * blocks + g_here
    ag5[slot_here] = jnp.where(line < qn, first, pltpu.roll(second, qn, 0)).astype(BF16)
    across_runs(lambda g: ag5.at[slot_here], ag5.at[slot_here], 6)
    wave(1)
    drain(ag5.at[pl.ds(0, blocks - 1)], s_recv.at[6])
    mates(lambda k: of_class(ag5, k_here), of_class(ag5, k_here), 7)
    wave(2)
    for load in loads[13:]:
        load.wait()
    drain(ag5.at[pl.ds(0, (near - 1) * blocks)], s_recv.at[7])

    wide[...] = ag5[...].astype(F32)
    acc = across(wide[:, 0, :].astype(BF16), wo[:, 0:HD])
    for g in range(1, n_rep * qn):
        acc = acc + across(wide[:, g, :].astype(BF16), wo[:, g * HD : (g + 1) * HD])
    pad = jnp.zeros((rows, HD - acc.shape[1]), F32)
    part6[h] = jnp.concatenate([acc, pad], axis=1)
    for t in range(1, n_head):
        peer = lax.rem(h + t, n_head)
        send(part6.at[h], part6.at[h], s_send.at[8], s_recv.at[8], head=peer)
    drain(part6.at[pl.ds(0, n_head - 1)], s_recv.at[8])
    proj = part6[0]
    for s in range(1, n_head):
        proj = proj + part6[s]
    middle = x + proj[:, : x.shape[1]]

    square = jnp.broadcast_to(jnp.sum(middle * middle, axis=1, keepdims=True), (rows, HD))
    y = both_parts(middle * fgain[...])
    fn = wg.shape[1] // n_rep // HD
    pg, pu = (folded(dot(y, w[...])) for w in (wg, wu))
    for side, buf in ((1, far7), (0, own7)):
        here = (r == 0) if side == 0 else (r != 0)
        for p, start in ((pg, 0), (pu, 8)):
            for c in range(fn):
                buf[:, start + c, :] = jnp.where(
                    here, p[:, c * HD : (c + 1) * HD], p[:, (fn + c) * HD : (fn + c + 1) * HD]
                )
            for c in range(fn, 8):
                buf[:, start + c, :] = square
        if side == 1:
            send(far7, got7, s_send.at[9], s_recv.at[9], rep=other)
    drain(got7, s_recv.at[9])
    own7[...] = own7[...] + got7[...]
    mates(lambda k: of_class(own7, k), near8.at[k_here], 10)
    near8[k_here] = own7[pl.ds(k_here * blocks, blocks)]
    wave(3)
    drain(near8.at[pl.ds(0, near - 1)], s_recv.at[10])
    total = jnp.sum(near8[...], axis=0)
    square = total[:, 7, :]
    near8[0] = total
    near8[0, :, 15, :] = square - square.astype(BF16).astype(F32)
    part8[...] = near8[0].astype(BF16)
    across_runs(lambda g: part8.at[g], row8.at[g_here], 11)
    row8[g_here] = part8[g_here]
    wave(4)

    drain(row8.at[pl.ds(0, blocks - 1)], s_recv.at[11])
    total = jnp.sum(row8[...].astype(F32), axis=0)
    scale = lax.rsqrt((total[7:8, 0:1] + total[15:16, 0:1]) / D + EPSILON)
    gate = total[0:8] * scale
    up = total[8:16] * scale
    hidden = gate / (1.0 + jnp.exp(-gate)) * up
    ag9[slot_here] = jnp.where(line < fn, hidden, 0.0).astype(BF16)
    across_runs(lambda g: ag9.at[slot_here], ag9.at[slot_here], 12)
    wave(5)
    drain(ag9.at[pl.ds(0, blocks - 1)], s_recv.at[12])
    mates(lambda k: of_class(ag9, k_here), of_class(ag9, k_here), 13)
    wave(6)
    drain(ag9.at[pl.ds(0, (near - 1) * blocks)], s_recv.at[13])
    send(ag9, pair9, s_send.at[14], s_recv.at[14], rep=other)

    def down(ref, which):
        wide[...] = ref[...].astype(F32)
        acc = jnp.zeros((rows, x.shape[1]), F32)
        for c in range(fn):
            start = pl.multiple_of((which * fn + c) * HD, HD)
            acc = acc + across(wide[:, c, :].astype(BF16), wd[:, pl.ds(start, HD)])
        return acc

    acc = down(ag9, r)
    drain(pair9, s_recv.at[14])
    acc = acc + down(pair9, other)
    part11[h] = jnp.concatenate([acc, pad], axis=1)
    for t in range(1, n_head):
        peer = lax.rem(h + t, n_head)
        send(part11.at[h], part11.at[h], s_send.at[15], s_recv.at[15], head=peer)
    drain(part11.at[pl.ds(0, n_head - 1)], s_recv.at[15])
    proj = part11[0]
    for s in range(1, n_head):
        proj = proj + part11[s]
    layer = (middle + proj[:, : x.shape[1]]).astype(BF16)
    layer_out[...] = lax.dot_general(
        to_row, layer, (((0,), (0,)), ((), ())), preferred_element_type=F32
    ).astype(BF16)

    for q in range(count):
        start = (q % pieces) * some
        here = z * BLK + r * half + start + lax.broadcasted_iota(jnp.int32, (some, width), 0)
        drain(arrived[q].at[pl.ds(0, n_seq - 1)], b_recv.at[q])

        def place(i, _):
            found = arrived[q][prow[i]]
            decoded[q // pieces, i, start : start + some, :] = jnp.where(
                here < lens[i], found, jnp.zeros((), found.dtype)
            )
            return 0

        lax.fori_loop(0, rows, place, 0)

    for q in range(count):
        drain(pool[q].at[pl.ds(0, (n_head - 1) * slots)], b_xsend.at[q])
        drain(ordered[q].at[pl.ds(0, n_seq - 1)], b_send.at[q])
    drain(far1, s_send.at[0])
    drain(near1.at[pl.ds(0, near - 1)], s_send.at[1])
    drain(row1.at[pl.ds(0, blocks - 1)], s_send.at[2])
    drain(tile3.at[pl.ds(0, n_kv - 1)], s_send.at[3])
    drain(state4.at[pl.ds(0, n_kv - 1)], s_send.at[4])
    drain(swap5, s_send.at[5])
    drain(ag5.at[pl.ds(0, blocks - 1)], s_send.at[6])
    drain(ag5.at[pl.ds(0, (near - 1) * blocks)], s_send.at[7])
    drain(part6.at[pl.ds(0, n_head - 1)], s_send.at[8])
    drain(far7, s_send.at[9])
    drain(near8.at[pl.ds(0, near - 1)], s_send.at[10])
    drain(row8.at[pl.ds(0, blocks - 1)], s_send.at[11])
    drain(ag9.at[pl.ds(0, blocks - 1)], s_send.at[12])
    drain(ag9.at[pl.ds(0, (near - 1) * blocks)], s_send.at[13])
    drain(ag9, s_send.at[14])
    drain(part11.at[pl.ds(0, n_head - 1)], s_send.at[15])


def angle_table(positions):
    turns = np.exp(np.arange(HD // 2) * (-2.0 * ROPE_LOG / HD))
    angles = positions[:, None] * np.concatenate([turns, turns])[None, :]
    return jnp.asarray(np.stack([np.cos(angles), np.sin(angles)], axis=1), F32)


def shards(
    tokens,
    attn_gain,
    ffn_gain,
    w_query,
    w_key,
    w_value,
    w_out,
    w_gate,
    w_up,
    w_down,
    kv_pool,
    lengths,
    pool_row,
    block_table,
):
    rows, features = tokens.shape
    n_seq, n_head, n_rep = (lax.axis_size(a) for a in ("seq", "head", "rep"))
    slots, half = kv_pool.shape[2:4]
    width = kv_pool.shape[4] // n_head
    n_kv = n_head * n_rep

    given = (
        tokens,
        pool_row[None, :],
        attn_gain[None, :],
        ffn_gain[None, :],
        angle_table(np.arange(BLK * block_table.shape[1] // STEP + 1) * STEP),
        angle_table(np.arange(STEP)),
        w_query,
        w_key,
        w_value,
        kv_pool,
        w_out.T,
        w_gate,
        w_up,
        w_down.T,
        block_table,
        pool_row,
        lengths,
    )
    vmem = pl.BlockSpec(memory_space=pltpu.VMEM)
    hbm = pl.BlockSpec(memory_space=pltpu.HBM)
    pieces, near = PIECES, 4
    blocks = n_seq // near
    pool = (n_head * slots, half // pieces, width)
    ring = (n_seq, half // pieces, width)
    line, lines = (rows, 8, HD), (rows, 16, HD)
    return pl.pallas_call(
        functools.partial(kernel, n_seq, n_head, n_rep, near, pieces),
        out_shape=(
            jax.ShapeDtypeStruct((rows, features), BF16),
            jax.ShapeDtypeStruct((2, rows, half, width), BF16),
        ),
        in_specs=[hbm] * len(given),
        out_specs=(vmem, vmem),
        scratch_shapes=[
            *(pltpu.VMEM(a.shape, a.dtype) for a in given[:9]),
            pltpu.VMEM((2, *kv_pool.shape[2:]), BF16),
            *(pltpu.VMEM(a.shape, a.dtype) for a in given[10:14]),
            *(pltpu.SMEM(a.shape, a.dtype) for a in given[14:]),
            *(pltpu.VMEM(pool, BF16) for _ in range(2 * pieces)),
            *(pltpu.VMEM(ring, BF16) for _ in range(4 * pieces)),
            *(pltpu.VMEM(line, F32) for _ in range(3)),
            pltpu.VMEM((near, blocks, 8, HD), F32),
            pltpu.VMEM((blocks, 8, HD), F32),
            pltpu.VMEM((blocks, 8, HD), F32),
            pltpu.VMEM((n_kv, 8, HD), F32),
            pltpu.VMEM((n_kv, 16, HD), F32),
            pltpu.VMEM((n_kv, 16, HD), F32),
            pltpu.VMEM((8, HD), F32),
            pltpu.VMEM((8, HD), F32),
            pltpu.VMEM(line, BF16),
            pltpu.VMEM(line, F32),
            pltpu.VMEM((n_head, rows, HD), F32),
            *(pltpu.VMEM(lines, F32) for _ in range(3)),
            pltpu.VMEM((near, blocks, 16, HD), F32),
            pltpu.VMEM((blocks, 16, HD), BF16),
            pltpu.VMEM((blocks, 16, HD), BF16),
            *(pltpu.VMEM(line, BF16) for _ in range(2)),
            pltpu.VMEM((n_head, rows, HD), F32),
            pltpu.SemaphoreType.DMA((16,)),
            pltpu.SemaphoreType.DMA((16,)),
            pltpu.SemaphoreType.DMA((len(given),)),
            *(pltpu.SemaphoreType.DMA((2 * pieces,)) for _ in range(4)),
        ],
        compiler_params=pltpu.CompilerParams(
            collective_id=0, has_side_effects=True, vmem_limit_bytes=40 * 1024 * 1024
        ),
        name="decode_layer",
    )(*(pltpu.with_memory_space_constraint(a, pltpu.HBM) for a in given))


def solution(mesh):
    in_specs = (
        P("groups", ("seq", "rep")),
        P(("seq", "rep")),
        P(("seq", "rep")),
        P(("seq", "rep"), "head"),
        P(("seq", "rep"), "head"),
        P(("seq", "rep"), "head"),
        P("head", ("seq", "rep")),
        P(("seq", "rep"), "head"),
        P(("seq", "rep"), "head"),
        P("head", ("seq", "rep")),
        P(None, ("groups", "seq"), "head", "rep", None),
        P("groups"),
        P("groups"),
        P("groups", None),
    )
    out_specs = (P("groups", ("seq", "rep")), P(None, "groups", ("seq", "rep"), "head"))
    return jax.shard_map(shards, mesh=mesh, in_specs=in_specs, out_specs=out_specs, check_vma=False)
```

```python
import functools
import math

import jax
import jax.numpy as jnp
import numpy as np
from jax import lax
from jax.experimental import pallas as pl
from jax.experimental.pallas import tpu as pltpu
from jax.sharding import PartitionSpec as P

D = 4096
H = 32
KVH = 8
HD = 128
BLK = 128

EPSILON = 1e-05
ROPE_LOG = math.log(500000.0)
FLOOR_SCORE = -1e30
STEP = 64
PIECES = 4
WAVES = ((0, 1), (2,), (3,), (4,), (5,), (6,), (7,))
MESH = pl.DeviceIdType.MESH
BF16 = jnp.bfloat16
F32 = jnp.float32


def send(src, dst, send_sem, recv_sem, **where):
    pltpu.make_async_remote_copy(
        src_ref=src,
        dst_ref=dst,
        send_sem=send_sem,
        recv_sem=recv_sem,
        device_id=where,
        device_id_type=MESH,
    ).start()


def drain(ref, sem):
    pltpu.make_async_copy(ref, ref, sem).wait()


def dot(a, b):
    return jnp.dot(a, b, preferred_element_type=F32)


def across(a, b):
    return lax.dot_general(a, b, (((1,), (1,)), ((), ())), preferred_element_type=F32)


def both_parts(value):
    lead = value.astype(BF16)
    rest = (value - lead.astype(F32)).astype(BF16)
    return jnp.concatenate([lead, rest], axis=0)


def folded(product):
    rows = product.shape[0] // 2
    return product[:rows] + product[rows:]


def kernel(n_seq, n_head, n_rep, near, pieces, *refs):
    (
        tok_h, pvec_h, again_h, fgain_h, far_h, fine_h, wq_h, wk_h, wv_h, kv_h, wo_h, wg_h, wu_h, wd_h,
        table_h, prow_h, lens_h,
        layer_out, decoded,
        tok, pvec, again, fgain, far, fine, wq, wk, wv, kv, wo, wg, wu, wd,
        table, prow, lens,
    ) = refs[:36]
    count = 2 * pieces
    pool, ordered, arrived = (refs[36 + k * count : 36 + (k + 1) * count] for k in range(3))
    (
        own1, far1, got1, near1, part1, row1, tile3, state4, got4, swap5, got5, ag5, wide,
        part6, own7, far7, got7, out8, near8, sum8, part8, row8, ag9, pair9, part11,
        s_send, s_recv, s_load, b_xsend, b_xrecv, b_send, b_recv, s_ready,
    ) = refs[36 + 3 * count :]
    z = lax.axis_index("seq")
    h = lax.axis_index("head")
    r = lax.axis_index("rep")
    other = 1 - r
    j = h * n_rep + r
    n_kv = n_head * n_rep
    rows = n_seq
    blocks = n_seq // near
    k_here, g_here = z % near, z // near
    slots = kv.shape[1]
    half = kv.shape[2]
    held = slots * half
    some = half // pieces
    width = decoded.shape[3]

    barrier = pltpu.get_barrier_semaphore()

    for d in (*range(1, near + 1), *range(-near, 0)):
        pl.semaphore_signal(
            barrier, inc=1, device_id={"seq": lax.rem(z + d + n_seq, n_seq)}, device_id_type=MESH
        )
    for t in range(1, n_kv):
        peer = lax.rem(j + t, n_kv)
        pl.semaphore_signal(
            barrier,
            inc=1,
            device_id={"head": peer // n_rep, "rep": peer % n_rep},
            device_id_type=MESH,
        )
    loads = [
        pltpu.make_async_copy(src, dst, s_load.at[k])
        for k, (src, dst) in enumerate(
            zip(
                (kv_h.at[:, 0], tok_h, pvec_h, again_h, fgain_h, far_h, fine_h, wq_h, wk_h, wv_h,
                 table_h, prow_h, lens_h, wo_h, wg_h, wu_h, wd_h),
                (kv, tok, pvec, again, fgain, far, fine, wq, wk, wv,
                 table, prow, lens, wo, wg, wu, wd),
            )
        )
    ]
    for load in loads:
        load.start()

    loads[0].wait()
    pl.semaphore_wait(barrier, 2 * near + n_kv - 1)

    def widen(step, n):
        for d in (step, n_seq - step):
            pl.semaphore_signal(
                s_ready.at[n], inc=1, device_id={"seq": lax.rem(z + d, n_seq)}, device_id_type=MESH
            )

    widen(near, 0)

    def columns(q, owner):
        return (
            q // pieces,
            slice(None),
            pl.ds((q % pieces) * some, some),
            pl.ds(pl.multiple_of(owner * width, width), width),
        )

    for q in range(count):
        for t in range(1, n_head):
            peer = lax.rem(h + t, n_head)
            send(
                kv.at[columns(q, peer)],
                pool[q].at[pl.ds(h * slots, slots)],
                b_xsend.at[q],
                b_xrecv.at[q],
                head=peer,
            )

    for load in loads[1:13]:
        load.wait()
    at = lax.broadcasted_iota(jnp.int32, (rows, rows), 0)
    to_row = (at % blocks) * near + at // blocks == pvec[...]
    to_row = to_row.astype(F32).astype(BF16)
    x = dot(to_row, tok[...])
    square = jnp.broadcast_to(jnp.sum(x * x, axis=1, keepdims=True), (rows, HD))
    y = both_parts(x * again[...])
    pq, pk, pv = (folded(dot(y, w[...])) for w in (wq, wk, wv))
    qn = pq.shape[1] // n_rep // HD
    for side, buf in ((1, far1), (0, own1)):
        mine = (r == 0) if side == 0 else (r != 0)
        for c in range(qn):
            buf[:, c, :] = jnp.where(
                mine, pq[:, c * HD : (c + 1) * HD], pq[:, (qn + c) * HD : (qn + c + 1) * HD]
            )
        buf[:, qn, :] = jnp.where(mine, pk[:, :HD], pk[:, HD:])
        buf[:, qn + 1, :] = jnp.where(mine, pv[:, :HD], pv[:, HD:])
        buf[:, qn + 2, :] = square
        buf[:, qn + 3, :] = jnp.zeros((rows, HD), F32)
        if side == 1:
            send(far1, got1, s_send.at[0], s_recv.at[0], rep=other)

    def mates(part_of, dst, which):
        for t in range(1, near):
            peer = lax.rem(k_here + t, near)
            send(
                part_of(peer), dst, s_send.at[which], s_recv.at[which], seq=g_here * near + peer
            )

    def across_runs(part_of, dst, which):
        for t in range(1, blocks):
            peer = lax.rem(g_here + t, blocks)
            send(
                part_of(peer), dst, s_send.at[which], s_recv.at[which], seq=peer * near + k_here
            )

    def of_class(ref, k):
        return ref.at[pl.ds(k * blocks, blocks)]

    rounds = s_ready.shape[0]
    for n in range(1, rounds):
        pl.semaphore_wait(s_ready.at[n - 1], 2)
        widen(near << n, n)
    drain(got1, s_recv.at[0])
    own1[...] = own1[...] + got1[...]
    mates(lambda k: of_class(own1, k), near1.at[k_here], 1)
    near1[k_here] = own1[pl.ds(k_here * blocks, blocks)]
    drain(near1.at[pl.ds(0, near - 1)], s_recv.at[1])
    part1[...] = jnp.sum(near1[...], axis=0)
    pl.semaphore_wait(s_ready.at[rounds - 1], 2)
    across_runs(lambda g: part1.at[g], row1.at[g_here], 2)
    row1[g_here] = part1[g_here]

    owner = lax.fori_loop(0, rows, lambda i, at: jnp.where(prow[i] == z, i, at), 0)
    length = lens[owner]

    def put_in_order(q):
        pool[q][pl.ds(h * slots, slots)] = kv[columns(q, h)]
        drain(pool[q].at[pl.ds(0, (n_head - 1) * slots)], b_xrecv.at[q])

        def one(b, _):
            ordered[q][b] = pool[q][table[owner, b]]
            return 0

        lax.fori_loop(0, n_seq, one, 0)
        arrived[q][z] = ordered[q][z]

    reach = n_seq // 2 + 1

    def bulk(q, lo, hi):
        def body(d, _):
            d = hi - 1 - d
            peer = lax.rem(z + d, n_seq)
            send(ordered[q].at[peer], arrived[q].at[z], b_send.at[q], b_recv.at[q], seq=peer)
            back = lax.rem(z + n_seq - d, n_seq)

            @pl.when(d * 2 != n_seq)
            def _():
                send(ordered[q].at[back], arrived[q].at[z], b_send.at[q], b_recv.at[q], seq=back)

            return 0

        lax.fori_loop(0, hi - lo, body, 0)

    def wave(n):
        for q in WAVES[n]:
            put_in_order(q)
            bulk(q, 1, reach)

    wave(0)

    slot_of = lax.broadcasted_iota(jnp.int32, (1, held), 1) // half
    place_of = lax.broadcasted_iota(jnp.int32, (1, held), 1) % half

    def note_block(b, at):
        return jnp.where(slot_of + h * slots == table[owner, b], b, at)

    block_of = lax.fori_loop(0, n_seq, note_block, jnp.zeros((1, held), jnp.int32))
    live = block_of * BLK + r * half + place_of < length

    drain(row1.at[pl.ds(0, blocks - 1)], s_recv.at[2])
    total = jnp.sum(row1[...], axis=0)
    scale = lax.rsqrt(total[qn + 2 : qn + 3, 0:1] / D + EPSILON)
    total = total * scale
    line = lax.broadcasted_iota(jnp.int32, (8, HD), 0)
    lane = lax.broadcasted_iota(jnp.int32, (8, HD), 1)
    whole, part = far[length // STEP], fine[length % STEP]
    cosine = whole[0:1] * part[0:1] - whole[1:2] * part[1:2]
    sine = whole[1:2] * part[0:1] + whole[0:1] * part[1:2]
    sine = jnp.where(lane < HD // 2, -sine, sine)
    turned = total * cosine + pltpu.roll(total, HD // 2, 1) * sine
    mine = jnp.where(line <= qn, turned, jnp.where(line == qn + 1, total, 0.0))
    mine = mine.astype(BF16).astype(F32)
    tile3[j] = mine
    for t in range(1, n_kv):
        peer = lax.rem(j + t, n_kv)
        send(
            tile3.at[j], tile3.at[j], s_send.at[3], s_recv.at[3],
            head=peer // n_rep, rep=peer % n_rep,
        )
    drain(tile3.at[pl.ds(0, n_kv - 1)], s_recv.at[3])

    factor = 1.0 / math.sqrt(HD)
    for g in range(n_kv):
        keys = kv[0, :, :, g * HD : (g + 1) * HD].reshape(held, HD)
        values = kv[1, :, :, g * HD : (g + 1) * HD].reshape(held, HD)
        scores = across(tile3[g].astype(BF16), keys) * factor
        scores = jnp.where(live, scores, FLOOR_SCORE)
        top = jnp.max(scores, axis=1, keepdims=True)
        weights = jnp.where(live, jnp.exp(scores - top), 0.0)
        mass = jnp.sum(weights, axis=1, keepdims=True)
        state4[g, 0:8, :] = dot(weights.astype(BF16), values)
        state4[g, 8:16, :] = jnp.where(lane < HD // 2, top, mass)
    for t in range(1, n_kv):
        peer = lax.rem(j + t, n_kv)
        send(
            state4.at[peer], got4.at[j], s_send.at[4], s_recv.at[4],
            head=peer // n_rep, rep=peer % n_rep,
        )
    got4[j] = state4[j]
    drain(got4.at[pl.ds(0, n_kv - 1)], s_recv.at[4])
    own_score = jnp.sum(mine * mine[qn : qn + 1, :], axis=1, keepdims=True) * factor
    top = own_score
    for s in range(n_kv):
        top = jnp.maximum(top, got4[s, 8:16, 0:1])
    own = jnp.exp(own_score - top)
    mass = own
    mixed = own * mine[qn + 1 : qn + 2, :]
    for s in range(n_kv):
        kept = jnp.exp(got4[s, 8:16, 0:1] - top)
        mass = mass + kept * got4[s, 8:16, HD // 2 : HD // 2 + 1]
        mixed = mixed + kept * got4[s, 0:8, :]
    swap5[...] = mixed / mass
    send(swap5, got5, s_send.at[5], s_recv.at[5], rep=other)
    drain(got5, s_recv.at[5])
    first = jnp.where(r == 0, swap5[...], got5[...])
    second = jnp.where(r == 0, got5[...], swap5[...])
    slot_here = k_here * blocks + g_here
    ag5[slot_here] = jnp.where(line < qn, first, pltpu.roll(second, qn, 0)).astype(BF16)
    across_runs(lambda g: ag5.at[slot_here], ag5.at[slot_here], 6)
    wave(1)
    drain(ag5.at[pl.ds(0, blocks - 1)], s_recv.at[6])
    mates(lambda k: of_class(ag5, k_here), of_class(ag5, k_here), 7)
    wave(2)
    for load in loads[13:]:
        load.wait()
    drain(ag5.at[pl.ds(0, (near - 1) * blocks)], s_recv.at[7])

    wide[...] = ag5[...].astype(F32)
    acc = across(wide[:, 0, :].astype(BF16), wo[:, 0:HD])
    for g in range(1, n_rep * qn):
        acc = acc + across(wide[:, g, :].astype(BF16), wo[:, g * HD : (g + 1) * HD])
    pad = jnp.zeros((rows, HD - acc.shape[1]), F32)
    part6[h] = jnp.concatenate([acc, pad], axis=1)
    for t in range(1, n_head):
        peer = lax.rem(h + t, n_head)
        send(part6.at[h], part6.at[h], s_send.at[8], s_recv.at[8], head=peer)
    drain(part6.at[pl.ds(0, n_head - 1)], s_recv.at[8])
    proj = part6[0]
    for s in range(1, n_head):
        proj = proj + part6[s]
    middle = x + proj[:, : x.shape[1]]

    square = jnp.broadcast_to(jnp.sum(middle * middle, axis=1, keepdims=True), (rows, HD))
    y = both_parts(middle * fgain[...])
    fn = wg.shape[1] // n_rep // HD
    pg, pu = (folded(dot(y, w[...])) for w in (wg, wu))
    for side, buf in ((1, far7), (0, own7)):
        here = (r == 0) if side == 0 else (r != 0)
        for p, start in ((pg, 0), (pu, 8)):
            for c in range(fn):
                buf[:, start + c, :] = jnp.where(
                    here, p[:, c * HD : (c + 1) * HD], p[:, (fn + c) * HD : (fn + c + 1) * HD]
                )
            for c in range(fn, 8):
                buf[:, start + c, :] = square
        if side == 1:
            send(far7, got7, s_send.at[9], s_recv.at[9], rep=other)
    drain(got7, s_recv.at[9])
    own7[...] = own7[...] + got7[...]
    square = own7[:, 7, :]
    own7[:, 15, :] = square - square.astype(BF16).astype(F32)
    out8[...] = own7[...].astype(BF16)
    mates(lambda k: of_class(out8, k), near8.at[k_here], 10)
    near8[k_here] = out8[pl.ds(k_here * blocks, blocks)]
    wave(3)
    drain(near8.at[pl.ds(0, near - 1)], s_recv.at[10])
    sum8[...] = jnp.sum(near8[...].astype(F32), axis=0)
    square = sum8[:, 7, :] + sum8[:, 15, :]
    sum8[:, 7, :] = square
    sum8[:, 15, :] = square - square.astype(BF16).astype(F32)
    part8[...] = sum8[...].astype(BF16)
    across_runs(lambda g: part8.at[g], row8.at[g_here], 11)
    row8[g_here] = part8[g_here]
    wave(4)

    drain(row8.at[pl.ds(0, blocks - 1)], s_recv.at[11])
    total = jnp.sum(row8[...].astype(F32), axis=0)
    scale = lax.rsqrt((total[7:8, 0:1] + total[15:16, 0:1]) / D + EPSILON)
    gate = total[0:8] * scale
    up = total[8:16] * scale
    hidden = gate / (1.0 + jnp.exp(-gate)) * up
    ag9[slot_here] = jnp.where(line < fn, hidden, 0.0).astype(BF16)
    across_runs(lambda g: ag9.at[slot_here], ag9.at[slot_here], 12)
    wave(5)
    drain(ag9.at[pl.ds(0, blocks - 1)], s_recv.at[12])
    mates(lambda k: of_class(ag9, k_here), of_class(ag9, k_here), 13)
    wave(6)
    drain(ag9.at[pl.ds(0, (near - 1) * blocks)], s_recv.at[13])
    send(ag9, pair9, s_send.at[14], s_recv.at[14], rep=other)

    def down(ref, which):
        wide[...] = ref[...].astype(F32)
        acc = jnp.zeros((rows, x.shape[1]), F32)
        for c in range(fn):
            start = pl.multiple_of((which * fn + c) * HD, HD)
            acc = acc + across(wide[:, c, :].astype(BF16), wd[:, pl.ds(start, HD)])
        return acc

    acc = down(ag9, r)
    drain(pair9, s_recv.at[14])
    acc = acc + down(pair9, other)
    part11[h] = jnp.concatenate([acc, pad], axis=1)
    for t in range(1, n_head):
        peer = lax.rem(h + t, n_head)
        send(part11.at[h], part11.at[h], s_send.at[15], s_recv.at[15], head=peer)
    drain(part11.at[pl.ds(0, n_head - 1)], s_recv.at[15])
    proj = part11[0]
    for s in range(1, n_head):
        proj = proj + part11[s]
    layer = (middle + proj[:, : x.shape[1]]).astype(BF16)
    layer_out[...] = lax.dot_general(
        to_row, layer, (((0,), (0,)), ((), ())), preferred_element_type=F32
    ).astype(BF16)

    for q in range(count):
        start = (q % pieces) * some
        here = z * BLK + r * half + start + lax.broadcasted_iota(jnp.int32, (some, width), 0)
        drain(arrived[q].at[pl.ds(0, n_seq - 1)], b_recv.at[q])

        def place(i, _):
            found = arrived[q][prow[i]]
            decoded[q // pieces, i, start : start + some, :] = jnp.where(
                here < lens[i], found, jnp.zeros((), found.dtype)
            )
            return 0

        lax.fori_loop(0, rows, place, 0)

    for q in range(count):
        drain(pool[q].at[pl.ds(0, (n_head - 1) * slots)], b_xsend.at[q])
        drain(ordered[q].at[pl.ds(0, n_seq - 1)], b_send.at[q])
    drain(far1, s_send.at[0])
    drain(near1.at[pl.ds(0, near - 1)], s_send.at[1])
    drain(row1.at[pl.ds(0, blocks - 1)], s_send.at[2])
    drain(tile3.at[pl.ds(0, n_kv - 1)], s_send.at[3])
    drain(state4.at[pl.ds(0, n_kv - 1)], s_send.at[4])
    drain(swap5, s_send.at[5])
    drain(ag5.at[pl.ds(0, blocks - 1)], s_send.at[6])
    drain(ag5.at[pl.ds(0, (near - 1) * blocks)], s_send.at[7])
    drain(part6.at[pl.ds(0, n_head - 1)], s_send.at[8])
    drain(far7, s_send.at[9])
    drain(near8.at[pl.ds(0, near - 1)], s_send.at[10])
    drain(row8.at[pl.ds(0, blocks - 1)], s_send.at[11])
    drain(ag9.at[pl.ds(0, blocks - 1)], s_send.at[12])
    drain(ag9.at[pl.ds(0, (near - 1) * blocks)], s_send.at[13])
    drain(ag9, s_send.at[14])
    drain(part11.at[pl.ds(0, n_head - 1)], s_send.at[15])


def angle_table(positions):
    turns = np.exp(np.arange(HD // 2) * (-2.0 * ROPE_LOG / HD))
    angles = positions[:, None] * np.concatenate([turns, turns])[None, :]
    return jnp.asarray(np.stack([np.cos(angles), np.sin(angles)], axis=1), F32)


def shards(
    tokens,
    attn_gain,
    ffn_gain,
    w_query,
    w_key,
    w_value,
    w_out,
    w_gate,
    w_up,
    w_down,
    kv_pool,
    lengths,
    pool_row,
    block_table,
):
    rows, features = tokens.shape
    n_seq, n_head, n_rep = (lax.axis_size(a) for a in ("seq", "head", "rep"))
    slots, half = kv_pool.shape[2:4]
    width = kv_pool.shape[4] // n_head
    n_kv = n_head * n_rep

    given = (
        tokens,
        pool_row[None, :],
        attn_gain[None, :],
        ffn_gain[None, :],
        angle_table(np.arange(BLK * block_table.shape[1] // STEP + 1) * STEP),
        angle_table(np.arange(STEP)),
        w_query,
        w_key,
        w_value,
        kv_pool,
        w_out.T,
        w_gate,
        w_up,
        w_down.T,
        block_table,
        pool_row,
        lengths,
    )
    vmem = pl.BlockSpec(memory_space=pltpu.VMEM)
    hbm = pl.BlockSpec(memory_space=pltpu.HBM)
    pieces, near = PIECES, 4
    rounds = (n_seq // (2 * near)).bit_length() - 1
    blocks = n_seq // near
    pool = (n_head * slots, half // pieces, width)
    ring = (n_seq, half // pieces, width)
    line, lines = (rows, 8, HD), (rows, 16, HD)
    return pl.pallas_call(
        functools.partial(kernel, n_seq, n_head, n_rep, near, pieces),
        out_shape=(
            jax.ShapeDtypeStruct((rows, features), BF16),
            jax.ShapeDtypeStruct((2, rows, half, width), BF16),
        ),
        in_specs=[hbm] * len(given),
        out_specs=(vmem, vmem),
        scratch_shapes=[
            *(pltpu.VMEM(a.shape, a.dtype) for a in given[:9]),
            pltpu.VMEM((2, *kv_pool.shape[2:]), BF16),
            *(pltpu.VMEM(a.shape, a.dtype) for a in given[10:14]),
            *(pltpu.SMEM(a.shape, a.dtype) for a in given[14:]),
            *(pltpu.VMEM(pool, BF16) for _ in range(2 * pieces)),
            *(pltpu.VMEM(ring, BF16) for _ in range(4 * pieces)),
            *(pltpu.VMEM(line, F32) for _ in range(3)),
            pltpu.VMEM((near, blocks, 8, HD), F32),
            pltpu.VMEM((blocks, 8, HD), F32),
            pltpu.VMEM((blocks, 8, HD), F32),
            pltpu.VMEM((n_kv, 8, HD), F32),
            pltpu.VMEM((n_kv, 16, HD), F32),
            pltpu.VMEM((n_kv, 16, HD), F32),
            pltpu.VMEM((8, HD), F32),
            pltpu.VMEM((8, HD), F32),
            pltpu.VMEM(line, BF16),
            pltpu.VMEM(line, F32),
            pltpu.VMEM((n_head, rows, HD), F32),
            *(pltpu.VMEM(lines, F32) for _ in range(3)),
            pltpu.VMEM(lines, BF16),
            pltpu.VMEM((near, blocks, 16, HD), BF16),
            pltpu.VMEM((blocks, 16, HD), F32),
            pltpu.VMEM((blocks, 16, HD), BF16),
            pltpu.VMEM((blocks, 16, HD), BF16),
            *(pltpu.VMEM(line, BF16) for _ in range(2)),
            pltpu.VMEM((n_head, rows, HD), F32),
            pltpu.SemaphoreType.DMA((16,)),
            pltpu.SemaphoreType.DMA((16,)),
            pltpu.SemaphoreType.DMA((len(given),)),
            *(pltpu.SemaphoreType.DMA((2 * pieces,)) for _ in range(4)),
            pltpu.SemaphoreType.REGULAR((rounds,)),
        ],
        compiler_params=pltpu.CompilerParams(
            collective_id=0, has_side_effects=True, vmem_limit_bytes=40 * 1024 * 1024
        ),
        name="decode_layer",
    )(*(pltpu.with_memory_space_constraint(a, pltpu.HBM) for a in given))


def solution(mesh):
    in_specs = (
        P("groups", ("seq", "rep")),
        P(("seq", "rep")),
        P(("seq", "rep")),
        P(("seq", "rep"), "head"),
        P(("seq", "rep"), "head"),
        P(("seq", "rep"), "head"),
        P("head", ("seq", "rep")),
        P(("seq", "rep"), "head"),
        P(("seq", "rep"), "head"),
        P("head", ("seq", "rep")),
        P(None, ("groups", "seq"), "head", "rep", None),
        P("groups"),
        P("groups"),
        P("groups", None),
    )
    out_specs = (P("groups", ("seq", "rep")), P(None, "groups", ("seq", "rep"), "head"))
    return jax.shard_map(shards, mesh=mesh, in_specs=in_specs, out_specs=out_specs, check_vma=False)
```

```python
import functools
import math

import jax
import jax.numpy as jnp
import numpy as np
from jax import lax
from jax.experimental import pallas as pl
from jax.experimental.pallas import tpu as pltpu
from jax.sharding import PartitionSpec as P

D = 4096
H = 32
KVH = 8
HD = 128
BLK = 128

EPSILON = 1e-05
ROPE_LOG = math.log(500000.0)
FLOOR_SCORE = -1e30
STEP = 64
PIECES = 4
WAVES = ((1,), (2,), (3,), (4,), (5,), (6,), (7,))
MESH = pl.DeviceIdType.MESH
BF16 = jnp.bfloat16
F32 = jnp.float32


def send(src, dst, send_sem, recv_sem, **where):
    pltpu.make_async_remote_copy(
        src_ref=src,
        dst_ref=dst,
        send_sem=send_sem,
        recv_sem=recv_sem,
        device_id=where,
        device_id_type=MESH,
    ).start()


def drain(ref, sem):
    pltpu.make_async_copy(ref, ref, sem).wait()


def dot(a, b):
    return jnp.dot(a, b, preferred_element_type=F32)


def across(a, b):
    return lax.dot_general(a, b, (((1,), (1,)), ((), ())), preferred_element_type=F32)


def both_parts(value):
    lead = value.astype(BF16)
    rest = (value - lead.astype(F32)).astype(BF16)
    return jnp.concatenate([lead, rest], axis=0)


def folded(product):
    rows = product.shape[0] // 2
    return product[:rows] + product[rows:]


def kernel(n_seq, n_head, n_rep, near, pieces, *refs):
    (
        tok_h, pvec_h, again_h, fgain_h, far_h, fine_h, wq_h, wk_h, wv_h, kv_h, wo_h, wg_h, wu_h, wd_h,
        table_h, prow_h, lens_h,
        layer_out, decoded,
        tok, pvec, again, fgain, far, fine, wq, wk, wv, kv, wo, wg, wu, wd,
        table, prow, lens,
    ) = refs[:36]
    count = 2 * pieces
    pool, ordered, arrived = (refs[36 + k * count : 36 + (k + 1) * count] for k in range(3))
    (
        own1, far1, got1, near1, part1, row1, tile3, state4, got4, swap5, got5, ag5, wide,
        part6, own7, far7, got7, out8, near8, sum8, part8, row8, ag9, pair9, part11,
        s_send, s_recv, s_load, b_xsend, b_xrecv, b_send, b_recv, s_ready,
    ) = refs[36 + 3 * count :]
    z = lax.axis_index("seq")
    h = lax.axis_index("head")
    r = lax.axis_index("rep")
    other = 1 - r
    j = h * n_rep + r
    n_kv = n_head * n_rep
    rows = n_seq
    blocks = n_seq // near
    k_here, g_here = z % near, z // near
    slots = kv.shape[1]
    half = kv.shape[2]
    held = slots * half
    some = half // pieces
    width = decoded.shape[3]

    barrier = pltpu.get_barrier_semaphore()

    for d in (*range(1, near + 1), *range(-near, 0)):
        pl.semaphore_signal(
            barrier, inc=1, device_id={"seq": lax.rem(z + d + n_seq, n_seq)}, device_id_type=MESH
        )
    for t in range(1, n_kv):
        peer = lax.rem(j + t, n_kv)
        pl.semaphore_signal(
            barrier,
            inc=1,
            device_id={"head": peer // n_rep, "rep": peer % n_rep},
            device_id_type=MESH,
        )
    loads = [
        pltpu.make_async_copy(src, dst, s_load.at[k])
        for k, (src, dst) in enumerate(
            zip(
                (kv_h.at[:, 0], tok_h, pvec_h, again_h, fgain_h, far_h, fine_h, wq_h, wk_h, wv_h,
                 table_h, prow_h, lens_h, wo_h, wg_h, wu_h, wd_h),
                (kv, tok, pvec, again, fgain, far, fine, wq, wk, wv,
                 table, prow, lens, wo, wg, wu, wd),
            )
        )
    ]
    for load in loads:
        load.start()

    loads[0].wait()
    pl.semaphore_wait(barrier, 2 * near + n_kv - 1)

    def widen(step, n):
        for d in (step, n_seq - step):
            pl.semaphore_signal(
                s_ready.at[n], inc=1, device_id={"seq": lax.rem(z + d, n_seq)}, device_id_type=MESH
            )

    widen(near, 0)

    def columns(q, owner):
        return (
            q // pieces,
            slice(None),
            pl.ds((q % pieces) * some, some),
            pl.ds(pl.multiple_of(owner * width, width), width),
        )

    for q in range(count):
        for t in range(1, n_head):
            peer = lax.rem(h + t, n_head)
            send(
                kv.at[columns(q, peer)],
                pool[q].at[pl.ds(h * slots, slots)],
                b_xsend.at[q],
                b_xrecv.at[q],
                head=peer,
            )

    for load in loads[1:13]:
        load.wait()
    at = lax.broadcasted_iota(jnp.int32, (rows, rows), 0)
    to_row = (at % blocks) * near + at // blocks == pvec[...]
    to_row = to_row.astype(F32).astype(BF16)
    x = dot(to_row, tok[...])
    square = jnp.broadcast_to(jnp.sum(x * x, axis=1, keepdims=True), (rows, HD))
    y = both_parts(x * again[...])
    pq, pk, pv = (folded(dot(y, w[...])) for w in (wq, wk, wv))
    qn = pq.shape[1] // n_rep // HD
    for side, buf in ((1, far1), (0, own1)):
        mine = (r == 0) if side == 0 else (r != 0)
        for c in range(qn):
            buf[:, c, :] = jnp.where(
                mine, pq[:, c * HD : (c + 1) * HD], pq[:, (qn + c) * HD : (qn + c + 1) * HD]
            )
        buf[:, qn, :] = jnp.where(mine, pk[:, :HD], pk[:, HD:])
        buf[:, qn + 1, :] = jnp.where(mine, pv[:, :HD], pv[:, HD:])
        buf[:, qn + 2, :] = square
        buf[:, qn + 3, :] = jnp.zeros((rows, HD), F32)
        if side == 1:
            send(far1, got1, s_send.at[0], s_recv.at[0], rep=other)

    def mates(part_of, dst, which):
        for t in range(1, near):
            peer = lax.rem(k_here + t, near)
            send(
                part_of(peer), dst, s_send.at[which], s_recv.at[which], seq=g_here * near + peer
            )

    def across_runs(part_of, dst, which):
        for t in range(1, blocks):
            peer = lax.rem(g_here + t, blocks)
            send(
                part_of(peer), dst, s_send.at[which], s_recv.at[which], seq=peer * near + k_here
            )

    def of_class(ref, k):
        return ref.at[pl.ds(k * blocks, blocks)]

    owner = lax.fori_loop(0, rows, lambda i, at: jnp.where(prow[i] == z, i, at), 0)
    length = lens[owner]

    rounds = s_ready.shape[0]
    for n in range(1, rounds):
        pl.semaphore_wait(s_ready.at[n - 1], 2)
        widen(near << n, n)
    drain(got1, s_recv.at[0])
    own1[...] = own1[...] + got1[...]
    mates(lambda k: of_class(own1, k), near1.at[k_here], 1)
    near1[k_here] = own1[pl.ds(k_here * blocks, blocks)]

    def put_in_order(q):
        pool[q][pl.ds(h * slots, slots)] = kv[columns(q, h)]
        drain(pool[q].at[pl.ds(0, (n_head - 1) * slots)], b_xrecv.at[q])

        def one(b, _):
            ordered[q][b] = pool[q][table[owner, b]]
            return 0

        lax.fori_loop(0, n_seq, one, 0)
        arrived[q][z] = ordered[q][z]

    reach = n_seq // 2 + 1

    def bulk(q, lo, hi):
        def body(d, _):
            d = hi - 1 - d
            peer = lax.rem(z + d, n_seq)
            send(ordered[q].at[peer], arrived[q].at[z], b_send.at[q], b_recv.at[q], seq=peer)
            back = lax.rem(z + n_seq - d, n_seq)

            @pl.when(d * 2 != n_seq)
            def _():
                send(ordered[q].at[back], arrived[q].at[z], b_send.at[q], b_recv.at[q], seq=back)

            return 0

        lax.fori_loop(0, hi - lo, body, 0)

    def wave(n):
        for q in WAVES[n]:
            put_in_order(q)
            bulk(q, 1, reach)

    known = near << (rounds - 1)
    put_in_order(0)
    bulk(0, 1, known + 1)
    drain(near1.at[pl.ds(0, near - 1)], s_recv.at[1])
    part1[...] = jnp.sum(near1[...], axis=0)
    pl.semaphore_wait(s_ready.at[rounds - 1], 2)
    across_runs(lambda g: part1.at[g], row1.at[g_here], 2)
    row1[g_here] = part1[g_here]

    bulk(0, known + 1, reach)
    wave(0)

    slot_of = lax.broadcasted_iota(jnp.int32, (1, held), 1) // half
    place_of = lax.broadcasted_iota(jnp.int32, (1, held), 1) % half

    def note_block(b, at):
        return jnp.where(slot_of + h * slots == table[owner, b], b, at)

    block_of = lax.fori_loop(0, n_seq, note_block, jnp.zeros((1, held), jnp.int32))
    live = block_of * BLK + r * half + place_of < length

    drain(row1.at[pl.ds(0, blocks - 1)], s_recv.at[2])
    total = jnp.sum(row1[...], axis=0)
    scale = lax.rsqrt(total[qn + 2 : qn + 3, 0:1] / D + EPSILON)
    total = total * scale
    line = lax.broadcasted_iota(jnp.int32, (8, HD), 0)
    lane = lax.broadcasted_iota(jnp.int32, (8, HD), 1)
    whole, part = far[length // STEP], fine[length % STEP]
    cosine = whole[0:1] * part[0:1] - whole[1:2] * part[1:2]
    sine = whole[1:2] * part[0:1] + whole[0:1] * part[1:2]
    sine = jnp.where(lane < HD // 2, -sine, sine)
    turned = total * cosine + pltpu.roll(total, HD // 2, 1) * sine
    mine = jnp.where(line <= qn, turned, jnp.where(line == qn + 1, total, 0.0))
    mine = mine.astype(BF16).astype(F32)
    tile3[j] = mine
    for t in range(1, n_kv):
        peer = lax.rem(j + t, n_kv)
        send(
            tile3.at[j], tile3.at[j], s_send.at[3], s_recv.at[3],
            head=peer // n_rep, rep=peer % n_rep,
        )
    drain(tile3.at[pl.ds(0, n_kv - 1)], s_recv.at[3])

    factor = 1.0 / math.sqrt(HD)
    for g in range(n_kv):
        keys = kv[0, :, :, g * HD : (g + 1) * HD].reshape(held, HD)
        values = kv[1, :, :, g * HD : (g + 1) * HD].reshape(held, HD)
        scores = across(tile3[g].astype(BF16), keys) * factor
        scores = jnp.where(live, scores, FLOOR_SCORE)
        top = jnp.max(scores, axis=1, keepdims=True)
        weights = jnp.where(live, jnp.exp(scores - top), 0.0)
        mass = jnp.sum(weights, axis=1, keepdims=True)
        state4[g, 0:8, :] = dot(weights.astype(BF16), values)
        state4[g, 8:16, :] = jnp.where(lane < HD // 2, top, mass)
    for t in range(1, n_kv):
        peer = lax.rem(j + t, n_kv)
        send(
            state4.at[peer], got4.at[j], s_send.at[4], s_recv.at[4],
            head=peer // n_rep, rep=peer % n_rep,
        )
    got4[j] = state4[j]
    drain(got4.at[pl.ds(0, n_kv - 1)], s_recv.at[4])
    own_score = jnp.sum(mine * mine[qn : qn + 1, :], axis=1, keepdims=True) * factor
    top = own_score
    for s in range(n_kv):
        top = jnp.maximum(top, got4[s, 8:16, 0:1])
    own = jnp.exp(own_score - top)
    mass = own
    mixed = own * mine[qn + 1 : qn + 2, :]
    for s in range(n_kv):
        kept = jnp.exp(got4[s, 8:16, 0:1] - top)
        mass = mass + kept * got4[s, 8:16, HD // 2 : HD // 2 + 1]
        mixed = mixed + kept * got4[s, 0:8, :]
    swap5[...] = mixed / mass
    send(swap5, got5, s_send.at[5], s_recv.at[5], rep=other)
    drain(got5, s_recv.at[5])
    first = jnp.where(r == 0, swap5[...], got5[...])
    second = jnp.where(r == 0, got5[...], swap5[...])
    slot_here = k_here * blocks + g_here
    ag5[slot_here] = jnp.where(line < qn, first, pltpu.roll(second, qn, 0)).astype(BF16)
    across_runs(lambda g: ag5.at[slot_here], ag5.at[slot_here], 6)
    wave(1)
    drain(ag5.at[pl.ds(0, blocks - 1)], s_recv.at[6])
    mates(lambda k: of_class(ag5, k_here), of_class(ag5, k_here), 7)
    wave(2)
    for load in loads[13:]:
        load.wait()
    drain(ag5.at[pl.ds(0, (near - 1) * blocks)], s_recv.at[7])

    wide[...] = ag5[...].astype(F32)
    acc = across(wide[:, 0, :].astype(BF16), wo[:, 0:HD])
    for g in range(1, n_rep * qn):
        acc = acc + across(wide[:, g, :].astype(BF16), wo[:, g * HD : (g + 1) * HD])
    pad = jnp.zeros((rows, HD - acc.shape[1]), F32)
    part6[h] = jnp.concatenate([acc, pad], axis=1)
    for t in range(1, n_head):
        peer = lax.rem(h + t, n_head)
        send(part6.at[h], part6.at[h], s_send.at[8], s_recv.at[8], head=peer)
    drain(part6.at[pl.ds(0, n_head - 1)], s_recv.at[8])
    proj = part6[0]
    for s in range(1, n_head):
        proj = proj + part6[s]
    middle = x + proj[:, : x.shape[1]]

    square = jnp.broadcast_to(jnp.sum(middle * middle, axis=1, keepdims=True), (rows, HD))
    y = both_parts(middle * fgain[...])
    fn = wg.shape[1] // n_rep // HD
    pg, pu = (folded(dot(y, w[...])) for w in (wg, wu))
    for side, buf in ((1, far7), (0, own7)):
        here = (r == 0) if side == 0 else (r != 0)
        for p, start in ((pg, 0), (pu, 8)):
            for c in range(fn):
                buf[:, start + c, :] = jnp.where(
                    here, p[:, c * HD : (c + 1) * HD], p[:, (fn + c) * HD : (fn + c + 1) * HD]
                )
            for c in range(fn, 8):
                buf[:, start + c, :] = square
        if side == 1:
            send(far7, got7, s_send.at[9], s_recv.at[9], rep=other)
    drain(got7, s_recv.at[9])
    own7[...] = own7[...] + got7[...]
    square = own7[:, 7, :]
    own7[:, 15, :] = square - square.astype(BF16).astype(F32)
    out8[...] = own7[...].astype(BF16)
    mates(lambda k: of_class(out8, k), near8.at[k_here], 10)
    near8[k_here] = out8[pl.ds(k_here * blocks, blocks)]
    wave(3)
    drain(near8.at[pl.ds(0, near - 1)], s_recv.at[10])
    sum8[...] = jnp.sum(near8[...].astype(F32), axis=0)
    square = sum8[:, 7, :] + sum8[:, 15, :]
    sum8[:, 7, :] = square
    sum8[:, 15, :] = square - square.astype(BF16).astype(F32)
    part8[...] = sum8[...].astype(BF16)
    across_runs(lambda g: part8.at[g], row8.at[g_here], 11)
    row8[g_here] = part8[g_here]
    wave(4)

    drain(row8.at[pl.ds(0, blocks - 1)], s_recv.at[11])
    total = jnp.sum(row8[...].astype(F32), axis=0)
    scale = lax.rsqrt((total[7:8, 0:1] + total[15:16, 0:1]) / D + EPSILON)
    gate = total[0:8] * scale
    up = total[8:16] * scale
    hidden = gate / (1.0 + jnp.exp(-gate)) * up
    ag9[slot_here] = jnp.where(line < fn, hidden, 0.0).astype(BF16)
    across_runs(lambda g: ag9.at[slot_here], ag9.at[slot_here], 12)
    wave(5)
    drain(ag9.at[pl.ds(0, blocks - 1)], s_recv.at[12])
    mates(lambda k: of_class(ag9, k_here), of_class(ag9, k_here), 13)
    wave(6)
    drain(ag9.at[pl.ds(0, (near - 1) * blocks)], s_recv.at[13])
    send(ag9, pair9, s_send.at[14], s_recv.at[14], rep=other)

    def down(ref, which):
        wide[...] = ref[...].astype(F32)
        acc = jnp.zeros((rows, x.shape[1]), F32)
        for c in range(fn):
            start = pl.multiple_of((which * fn + c) * HD, HD)
            acc = acc + across(wide[:, c, :].astype(BF16), wd[:, pl.ds(start, HD)])
        return acc

    acc = down(ag9, r)
    drain(pair9, s_recv.at[14])
    acc = acc + down(pair9, other)
    part11[h] = jnp.concatenate([acc, pad], axis=1)
    for t in range(1, n_head):
        peer = lax.rem(h + t, n_head)
        send(part11.at[h], part11.at[h], s_send.at[15], s_recv.at[15], head=peer)
    drain(part11.at[pl.ds(0, n_head - 1)], s_recv.at[15])
    proj = part11[0]
    for s in range(1, n_head):
        proj = proj + part11[s]
    layer = (middle + proj[:, : x.shape[1]]).astype(BF16)
    layer_out[...] = lax.dot_general(
        to_row, layer, (((0,), (0,)), ((), ())), preferred_element_type=F32
    ).astype(BF16)

    for q in range(count):
        start = (q % pieces) * some
        here = z * BLK + r * half + start + lax.broadcasted_iota(jnp.int32, (some, width), 0)
        drain(arrived[q].at[pl.ds(0, n_seq - 1)], b_recv.at[q])

        def place(i, _):
            found = arrived[q][prow[i]]
            decoded[q // pieces, i, start : start + some, :] = jnp.where(
                here < lens[i], found, jnp.zeros((), found.dtype)
            )
            return 0

        lax.fori_loop(0, rows, place, 0)

    for q in range(count):
        drain(pool[q].at[pl.ds(0, (n_head - 1) * slots)], b_xsend.at[q])
        drain(ordered[q].at[pl.ds(0, n_seq - 1)], b_send.at[q])
    drain(far1, s_send.at[0])
    drain(near1.at[pl.ds(0, near - 1)], s_send.at[1])
    drain(row1.at[pl.ds(0, blocks - 1)], s_send.at[2])
    drain(tile3.at[pl.ds(0, n_kv - 1)], s_send.at[3])
    drain(state4.at[pl.ds(0, n_kv - 1)], s_send.at[4])
    drain(swap5, s_send.at[5])
    drain(ag5.at[pl.ds(0, blocks - 1)], s_send.at[6])
    drain(ag5.at[pl.ds(0, (near - 1) * blocks)], s_send.at[7])
    drain(part6.at[pl.ds(0, n_head - 1)], s_send.at[8])
    drain(far7, s_send.at[9])
    drain(near8.at[pl.ds(0, near - 1)], s_send.at[10])
    drain(row8.at[pl.ds(0, blocks - 1)], s_send.at[11])
    drain(ag9.at[pl.ds(0, blocks - 1)], s_send.at[12])
    drain(ag9.at[pl.ds(0, (near - 1) * blocks)], s_send.at[13])
    drain(ag9, s_send.at[14])
    drain(part11.at[pl.ds(0, n_head - 1)], s_send.at[15])


def angle_table(positions):
    turns = np.exp(np.arange(HD // 2) * (-2.0 * ROPE_LOG / HD))
    angles = positions[:, None] * np.concatenate([turns, turns])[None, :]
    return jnp.asarray(np.stack([np.cos(angles), np.sin(angles)], axis=1), F32)


def shards(
    tokens,
    attn_gain,
    ffn_gain,
    w_query,
    w_key,
    w_value,
    w_out,
    w_gate,
    w_up,
    w_down,
    kv_pool,
    lengths,
    pool_row,
    block_table,
):
    rows, features = tokens.shape
    n_seq, n_head, n_rep = (lax.axis_size(a) for a in ("seq", "head", "rep"))
    slots, half = kv_pool.shape[2:4]
    width = kv_pool.shape[4] // n_head
    n_kv = n_head * n_rep

    given = (
        tokens,
        pool_row[None, :],
        attn_gain[None, :],
        ffn_gain[None, :],
        angle_table(np.arange(BLK * block_table.shape[1] // STEP + 1) * STEP),
        angle_table(np.arange(STEP)),
        w_query,
        w_key,
        w_value,
        kv_pool,
        w_out.T,
        w_gate,
        w_up,
        w_down.T,
        block_table,
        pool_row,
        lengths,
    )
    vmem = pl.BlockSpec(memory_space=pltpu.VMEM)
    hbm = pl.BlockSpec(memory_space=pltpu.HBM)
    pieces, near = PIECES, 4
    rounds = (n_seq // (2 * near)).bit_length() - 1
    blocks = n_seq // near
    pool = (n_head * slots, half // pieces, width)
    ring = (n_seq, half // pieces, width)
    line, lines = (rows, 8, HD), (rows, 16, HD)
    return pl.pallas_call(
        functools.partial(kernel, n_seq, n_head, n_rep, near, pieces),
        out_shape=(
            jax.ShapeDtypeStruct((rows, features), BF16),
            jax.ShapeDtypeStruct((2, rows, half, width), BF16),
        ),
        in_specs=[hbm] * len(given),
        out_specs=(vmem, vmem),
        scratch_shapes=[
            *(pltpu.VMEM(a.shape, a.dtype) for a in given[:9]),
            pltpu.VMEM((2, *kv_pool.shape[2:]), BF16),
            *(pltpu.VMEM(a.shape, a.dtype) for a in given[10:14]),
            *(pltpu.SMEM(a.shape, a.dtype) for a in given[14:]),
            *(pltpu.VMEM(pool, BF16) for _ in range(2 * pieces)),
            *(pltpu.VMEM(ring, BF16) for _ in range(4 * pieces)),
            *(pltpu.VMEM(line, F32) for _ in range(3)),
            pltpu.VMEM((near, blocks, 8, HD), F32),
            pltpu.VMEM((blocks, 8, HD), F32),
            pltpu.VMEM((blocks, 8, HD), F32),
            pltpu.VMEM((n_kv, 8, HD), F32),
            pltpu.VMEM((n_kv, 16, HD), F32),
            pltpu.VMEM((n_kv, 16, HD), F32),
            pltpu.VMEM((8, HD), F32),
            pltpu.VMEM((8, HD), F32),
            pltpu.VMEM(line, BF16),
            pltpu.VMEM(line, F32),
            pltpu.VMEM((n_head, rows, HD), F32),
            *(pltpu.VMEM(lines, F32) for _ in range(3)),
            pltpu.VMEM(lines, BF16),
            pltpu.VMEM((near, blocks, 16, HD), BF16),
            pltpu.VMEM((blocks, 16, HD), F32),
            pltpu.VMEM((blocks, 16, HD), BF16),
            pltpu.VMEM((blocks, 16, HD), BF16),
            *(pltpu.VMEM(line, BF16) for _ in range(2)),
            pltpu.VMEM((n_head, rows, HD), F32),
            pltpu.SemaphoreType.DMA((16,)),
            pltpu.SemaphoreType.DMA((16,)),
            pltpu.SemaphoreType.DMA((len(given),)),
            *(pltpu.SemaphoreType.DMA((2 * pieces,)) for _ in range(4)),
            pltpu.SemaphoreType.REGULAR((rounds,)),
        ],
        compiler_params=pltpu.CompilerParams(
            collective_id=0, has_side_effects=True, vmem_limit_bytes=40 * 1024 * 1024
        ),
        name="decode_layer",
    )(*(pltpu.with_memory_space_constraint(a, pltpu.HBM) for a in given))


def solution(mesh):
    in_specs = (
        P("groups", ("seq", "rep")),
        P(("seq", "rep")),
        P(("seq", "rep")),
        P(("seq", "rep"), "head"),
        P(("seq", "rep"), "head"),
        P(("seq", "rep"), "head"),
        P("head", ("seq", "rep")),
        P(("seq", "rep"), "head"),
        P(("seq", "rep"), "head"),
        P("head", ("seq", "rep")),
        P(None, ("groups", "seq"), "head", "rep", None),
        P("groups"),
        P("groups"),
        P("groups", None),
    )
    out_specs = (P("groups", ("seq", "rep")), P(None, "groups", ("seq", "rep"), "head"))
    return jax.shard_map(shards, mesh=mesh, in_specs=in_specs, out_specs=out_specs, check_vma=False)
```

```python
import functools
import math

import jax
import jax.numpy as jnp
import numpy as np
from jax import lax
from jax.experimental import pallas as pl
from jax.experimental.pallas import tpu as pltpu
from jax.sharding import PartitionSpec as P

D = 4096
H = 32
KVH = 8
HD = 128
BLK = 128

EPSILON = 1e-05
ROPE_LOG = math.log(500000.0)
FLOOR_SCORE = -1e30
STEP = 64
PIECES = 4
WAVES = (((1, 1), (2, 1)), ((3, 1),), ((4, 1),), ((5, 1),), ((6, 1),), ((7, 0),), ())
MESH = pl.DeviceIdType.MESH
BF16 = jnp.bfloat16
F32 = jnp.float32


def send(src, dst, send_sem, recv_sem, **where):
    pltpu.make_async_remote_copy(
        src_ref=src,
        dst_ref=dst,
        send_sem=send_sem,
        recv_sem=recv_sem,
        device_id=where,
        device_id_type=MESH,
    ).start()


def drain(ref, sem):
    pltpu.make_async_copy(ref, ref, sem).wait()


def dot(a, b):
    return jnp.dot(a, b, preferred_element_type=F32)


def across(a, b):
    return lax.dot_general(a, b, (((1,), (1,)), ((), ())), preferred_element_type=F32)


def both_parts(value):
    lead = value.astype(BF16)
    rest = (value - lead.astype(F32)).astype(BF16)
    return jnp.concatenate([lead, rest], axis=0)


def folded(product):
    rows = product.shape[0] // 2
    return product[:rows] + product[rows:]


def kernel(n_seq, n_head, n_rep, near, pieces, *refs):
    (
        tok_h, pvec_h, again_h, fgain_h, far_h, fine_h, wq_h, wk_h, wv_h, kv_h, wo_h, wg_h, wu_h, wd_h,
        table_h, prow_h, lens_h,
        layer_out, decoded,
        tok, pvec, again, fgain, far, fine, wq, wk, wv, kv, wo, wg, wu, wd,
        table, prow, lens,
    ) = refs[:36]
    count = 2 * pieces
    pool, ordered, arrived = (refs[36 + k * count : 36 + (k + 1) * count] for k in range(3))
    (
        own1, far1, got1, near1, part1, row1, tile3, state4, got4, swap5, got5, ag5, wide,
        part6, own7, far7, got7, out8, near8, sum8, part8, row8, ag9, pair9, part11,
        s_send, s_recv, s_load, b_xsend, b_xrecv, b_send, b_recv, s_ready,
    ) = refs[36 + 3 * count :]
    z = lax.axis_index("seq")
    h = lax.axis_index("head")
    r = lax.axis_index("rep")
    other = 1 - r
    j = h * n_rep + r
    n_kv = n_head * n_rep
    rows = n_seq
    blocks = n_seq // near
    k_here, g_here = z % near, z // near
    slots = kv.shape[1]
    half = kv.shape[2]
    held = slots * half
    some = half // pieces
    width = decoded.shape[3]

    barrier = pltpu.get_barrier_semaphore()

    for d in (*range(1, near + 1), *range(-near, 0)):
        pl.semaphore_signal(
            barrier, inc=1, device_id={"seq": lax.rem(z + d + n_seq, n_seq)}, device_id_type=MESH
        )
    for t in range(1, n_kv):
        peer = lax.rem(j + t, n_kv)
        pl.semaphore_signal(
            barrier,
            inc=1,
            device_id={"head": peer // n_rep, "rep": peer % n_rep},
            device_id_type=MESH,
        )
    loads = [
        pltpu.make_async_copy(src, dst, s_load.at[k])
        for k, (src, dst) in enumerate(
            zip(
                (kv_h.at[:, 0], tok_h, pvec_h, again_h, fgain_h, far_h, fine_h, wq_h, wk_h, wv_h,
                 table_h, prow_h, lens_h, wo_h, wg_h, wu_h, wd_h),
                (kv, tok, pvec, again, fgain, far, fine, wq, wk, wv,
                 table, prow, lens, wo, wg, wu, wd),
            )
        )
    ]
    for load in loads:
        load.start()

    loads[0].wait()
    pl.semaphore_wait(barrier, 2 * near + n_kv - 1)

    def widen(step, n):
        for d in (step, n_seq - step):
            pl.semaphore_signal(
                s_ready.at[n], inc=1, device_id={"seq": lax.rem(z + d, n_seq)}, device_id_type=MESH
            )

    widen(near, 0)

    def columns(q, owner):
        return (
            q // pieces,
            slice(None),
            pl.ds((q % pieces) * some, some),
            pl.ds(pl.multiple_of(owner * width, width), width),
        )

    for q in range(count):
        for t in range(1, n_head):
            peer = lax.rem(h + t, n_head)
            send(
                kv.at[columns(q, peer)],
                pool[q].at[pl.ds(h * slots, slots)],
                b_xsend.at[q],
                b_xrecv.at[q],
                head=peer,
            )

    for load in loads[1:13]:
        load.wait()
    at = lax.broadcasted_iota(jnp.int32, (rows, rows), 0)
    to_row = (at % blocks) * near + at // blocks == pvec[...]
    to_row = to_row.astype(F32).astype(BF16)
    x = dot(to_row, tok[...])
    square = jnp.broadcast_to(jnp.sum(x * x, axis=1, keepdims=True), (rows, HD))
    y = both_parts(x * again[...])
    pq, pk, pv = (folded(dot(y, w[...])) for w in (wq, wk, wv))
    qn = pq.shape[1] // n_rep // HD
    for side, buf in ((1, far1), (0, own1)):
        mine = (r == 0) if side == 0 else (r != 0)
        for c in range(qn):
            buf[:, c, :] = jnp.where(
                mine, pq[:, c * HD : (c + 1) * HD], pq[:, (qn + c) * HD : (qn + c + 1) * HD]
            )
        buf[:, qn, :] = jnp.where(mine, pk[:, :HD], pk[:, HD:])
        buf[:, qn + 1, :] = jnp.where(mine, pv[:, :HD], pv[:, HD:])
        buf[:, qn + 2, :] = square
        buf[:, qn + 3, :] = jnp.zeros((rows, HD), F32)
        if side == 1:
            send(far1, got1, s_send.at[0], s_recv.at[0], rep=other)

    def mates(part_of, dst, which):
        for t in range(1, near):
            peer = lax.rem(k_here + t, near)
            send(
                part_of(peer), dst, s_send.at[which], s_recv.at[which], seq=g_here * near + peer
            )

    def across_runs(part_of, dst, which):
        for t in range(1, blocks):
            peer = lax.rem(g_here + t, blocks)
            send(
                part_of(peer), dst, s_send.at[which], s_recv.at[which], seq=peer * near + k_here
            )

    def of_class(ref, k):
        return ref.at[pl.ds(k * blocks, blocks)]

    owner = lax.fori_loop(0, rows, lambda i, at: jnp.where(prow[i] == z, i, at), 0)
    length = lens[owner]

    rounds = s_ready.shape[0]
    for n in range(1, rounds):
        pl.semaphore_wait(s_ready.at[n - 1], 2)
        widen(near << n, n)
    drain(got1, s_recv.at[0])
    own1[...] = own1[...] + got1[...]
    mates(lambda k: of_class(own1, k), near1.at[k_here], 1)
    near1[k_here] = own1[pl.ds(k_here * blocks, blocks)]

    def put_in_order(q):
        pool[q][pl.ds(h * slots, slots)] = kv[columns(q, h)]
        drain(pool[q].at[pl.ds(0, (n_head - 1) * slots)], b_xrecv.at[q])

        def one(b, _):
            ordered[q][b] = pool[q][table[owner, b]]
            return 0

        lax.fori_loop(0, n_seq, one, 0)
        arrived[q][z] = ordered[q][z]

    reach = n_seq // 2 + 1
    known = near << (rounds - 1)

    def bulk(q, lo, hi):
        def body(d, _):
            d = hi - 1 - d
            peer = lax.rem(z + d, n_seq)
            send(ordered[q].at[peer], arrived[q].at[z], b_send.at[q], b_recv.at[q], seq=peer)
            back = lax.rem(z + n_seq - d, n_seq)

            @pl.when(d * 2 != n_seq)
            def _():
                send(ordered[q].at[back], arrived[q].at[z], b_send.at[q], b_recv.at[q], seq=back)

            return 0

        lax.fori_loop(0, hi - lo, body, 0)

    def wave(n):
        for q, near_too in WAVES[n]:
            put_in_order(q)
            bulk(q, 1 if near_too else known + 1, reach)

    put_in_order(0)
    bulk(0, 1, known + 1)
    drain(near1.at[pl.ds(0, near - 1)], s_recv.at[1])
    part1[...] = jnp.sum(near1[...], axis=0)
    pl.semaphore_wait(s_ready.at[rounds - 1], 2)
    across_runs(lambda g: part1.at[g], row1.at[g_here], 2)
    row1[g_here] = part1[g_here]

    bulk(0, known + 1, reach)
    wave(0)

    slot_of = lax.broadcasted_iota(jnp.int32, (1, held), 1) // half
    place_of = lax.broadcasted_iota(jnp.int32, (1, held), 1) % half

    def note_block(b, at):
        return jnp.where(slot_of + h * slots == table[owner, b], b, at)

    block_of = lax.fori_loop(0, n_seq, note_block, jnp.zeros((1, held), jnp.int32))
    live = block_of * BLK + r * half + place_of < length

    drain(row1.at[pl.ds(0, blocks - 1)], s_recv.at[2])
    total = jnp.sum(row1[...], axis=0)
    scale = lax.rsqrt(total[qn + 2 : qn + 3, 0:1] / D + EPSILON)
    total = total * scale
    line = lax.broadcasted_iota(jnp.int32, (8, HD), 0)
    lane = lax.broadcasted_iota(jnp.int32, (8, HD), 1)
    whole, part = far[length // STEP], fine[length % STEP]
    cosine = whole[0:1] * part[0:1] - whole[1:2] * part[1:2]
    sine = whole[1:2] * part[0:1] + whole[0:1] * part[1:2]
    sine = jnp.where(lane < HD // 2, -sine, sine)
    turned = total * cosine + pltpu.roll(total, HD // 2, 1) * sine
    mine = jnp.where(line <= qn, turned, jnp.where(line == qn + 1, total, 0.0))
    mine = mine.astype(BF16).astype(F32)
    tile3[j] = mine
    for t in range(1, n_kv):
        peer = lax.rem(j + t, n_kv)
        send(
            tile3.at[j], tile3.at[j], s_send.at[3], s_recv.at[3],
            head=peer // n_rep, rep=peer % n_rep,
        )
    drain(tile3.at[pl.ds(0, n_kv - 1)], s_recv.at[3])

    factor = 1.0 / math.sqrt(HD)
    for g in range(n_kv):
        keys = kv[0, :, :, g * HD : (g + 1) * HD].reshape(held, HD)
        values = kv[1, :, :, g * HD : (g + 1) * HD].reshape(held, HD)
        scores = across(tile3[g].astype(BF16), keys) * factor
        scores = jnp.where(live, scores, FLOOR_SCORE)
        top = jnp.max(scores, axis=1, keepdims=True)
        weights = jnp.where(live, jnp.exp(scores - top), 0.0)
        mass = jnp.sum(weights, axis=1, keepdims=True)
        state4[g, 0:8, :] = dot(weights.astype(BF16), values)
        state4[g, 8:16, :] = jnp.where(lane < HD // 2, top, mass)
    for t in range(1, n_kv):
        peer = lax.rem(j + t, n_kv)
        send(
            state4.at[peer], got4.at[j], s_send.at[4], s_recv.at[4],
            head=peer // n_rep, rep=peer % n_rep,
        )
    got4[j] = state4[j]
    drain(got4.at[pl.ds(0, n_kv - 1)], s_recv.at[4])
    own_score = jnp.sum(mine * mine[qn : qn + 1, :], axis=1, keepdims=True) * factor
    top = own_score
    for s in range(n_kv):
        top = jnp.maximum(top, got4[s, 8:16, 0:1])
    own = jnp.exp(own_score - top)
    mass = own
    mixed = own * mine[qn + 1 : qn + 2, :]
    for s in range(n_kv):
        kept = jnp.exp(got4[s, 8:16, 0:1] - top)
        mass = mass + kept * got4[s, 8:16, HD // 2 : HD // 2 + 1]
        mixed = mixed + kept * got4[s, 0:8, :]
    swap5[...] = mixed / mass
    send(swap5, got5, s_send.at[5], s_recv.at[5], rep=other)
    drain(got5, s_recv.at[5])
    first = jnp.where(r == 0, swap5[...], got5[...])
    second = jnp.where(r == 0, got5[...], swap5[...])
    slot_here = k_here * blocks + g_here
    ag5[slot_here] = jnp.where(line < qn, first, pltpu.roll(second, qn, 0)).astype(BF16)
    across_runs(lambda g: ag5.at[slot_here], ag5.at[slot_here], 6)
    wave(1)
    drain(ag5.at[pl.ds(0, blocks - 1)], s_recv.at[6])
    mates(lambda k: of_class(ag5, k_here), of_class(ag5, k_here), 7)
    wave(2)
    for load in loads[13:]:
        load.wait()
    drain(ag5.at[pl.ds(0, (near - 1) * blocks)], s_recv.at[7])

    wide[...] = ag5[...].astype(F32)
    acc = across(wide[:, 0, :].astype(BF16), wo[:, 0:HD])
    for g in range(1, n_rep * qn):
        acc = acc + across(wide[:, g, :].astype(BF16), wo[:, g * HD : (g + 1) * HD])
    pad = jnp.zeros((rows, HD - acc.shape[1]), F32)
    part6[h] = jnp.concatenate([acc, pad], axis=1)
    for t in range(1, n_head):
        peer = lax.rem(h + t, n_head)
        send(part6.at[h], part6.at[h], s_send.at[8], s_recv.at[8], head=peer)
    drain(part6.at[pl.ds(0, n_head - 1)], s_recv.at[8])
    proj = part6[0]
    for s in range(1, n_head):
        proj = proj + part6[s]
    middle = x + proj[:, : x.shape[1]]

    square = jnp.broadcast_to(jnp.sum(middle * middle, axis=1, keepdims=True), (rows, HD))
    y = both_parts(middle * fgain[...])
    fn = wg.shape[1] // n_rep // HD
    pg, pu = (folded(dot(y, w[...])) for w in (wg, wu))
    for side, buf in ((1, far7), (0, own7)):
        here = (r == 0) if side == 0 else (r != 0)
        for p, start in ((pg, 0), (pu, 8)):
            for c in range(fn):
                buf[:, start + c, :] = jnp.where(
                    here, p[:, c * HD : (c + 1) * HD], p[:, (fn + c) * HD : (fn + c + 1) * HD]
                )
            for c in range(fn, 8):
                buf[:, start + c, :] = square
        if side == 1:
            send(far7, got7, s_send.at[9], s_recv.at[9], rep=other)
    drain(got7, s_recv.at[9])
    own7[...] = own7[...] + got7[...]
    square = own7[:, 7, :]
    own7[:, 15, :] = square - square.astype(BF16).astype(F32)
    out8[...] = own7[...].astype(BF16)
    mates(lambda k: of_class(out8, k), near8.at[k_here], 10)
    near8[k_here] = out8[pl.ds(k_here * blocks, blocks)]
    wave(3)
    drain(near8.at[pl.ds(0, near - 1)], s_recv.at[10])
    sum8[...] = jnp.sum(near8[...].astype(F32), axis=0)
    square = sum8[:, 7, :] + sum8[:, 15, :]
    sum8[:, 7, :] = square
    sum8[:, 15, :] = square - square.astype(BF16).astype(F32)
    part8[...] = sum8[...].astype(BF16)
    across_runs(lambda g: part8.at[g], row8.at[g_here], 11)
    row8[g_here] = part8[g_here]
    wave(4)

    drain(row8.at[pl.ds(0, blocks - 1)], s_recv.at[11])
    total = jnp.sum(row8[...].astype(F32), axis=0)
    scale = lax.rsqrt((total[7:8, 0:1] + total[15:16, 0:1]) / D + EPSILON)
    gate = total[0:8] * scale
    up = total[8:16] * scale
    hidden = gate / (1.0 + jnp.exp(-gate)) * up
    ag9[slot_here] = jnp.where(line < fn, hidden, 0.0).astype(BF16)
    across_runs(lambda g: ag9.at[slot_here], ag9.at[slot_here], 12)
    wave(5)
    drain(ag9.at[pl.ds(0, blocks - 1)], s_recv.at[12])
    mates(lambda k: of_class(ag9, k_here), of_class(ag9, k_here), 13)
    wave(6)
    bulk(count - 1, 1, known + 1)
    drain(ag9.at[pl.ds(0, (near - 1) * blocks)], s_recv.at[13])
    send(ag9, pair9, s_send.at[14], s_recv.at[14], rep=other)

    def down(ref, which):
        wide[...] = ref[...].astype(F32)
        acc = jnp.zeros((rows, x.shape[1]), F32)
        for c in range(fn):
            start = pl.multiple_of((which * fn + c) * HD, HD)
            acc = acc + across(wide[:, c, :].astype(BF16), wd[:, pl.ds(start, HD)])
        return acc

    acc = down(ag9, r)
    drain(pair9, s_recv.at[14])
    acc = acc + down(pair9, other)
    part11[h] = jnp.concatenate([acc, pad], axis=1)
    for t in range(1, n_head):
        peer = lax.rem(h + t, n_head)
        send(part11.at[h], part11.at[h], s_send.at[15], s_recv.at[15], head=peer)
    drain(part11.at[pl.ds(0, n_head - 1)], s_recv.at[15])
    proj = part11[0]
    for s in range(1, n_head):
        proj = proj + part11[s]
    layer = (middle + proj[:, : x.shape[1]]).astype(BF16)
    layer_out[...] = lax.dot_general(
        to_row, layer, (((0,), (0,)), ((), ())), preferred_element_type=F32
    ).astype(BF16)

    for q in range(count):
        start = (q % pieces) * some
        here = z * BLK + r * half + start + lax.broadcasted_iota(jnp.int32, (some, width), 0)
        drain(arrived[q].at[pl.ds(0, n_seq - 1)], b_recv.at[q])

        def place(i, _):
            found = arrived[q][prow[i]]
            decoded[q // pieces, i, start : start + some, :] = jnp.where(
                here < lens[i], found, jnp.zeros((), found.dtype)
            )
            return 0

        lax.fori_loop(0, rows, place, 0)

    for q in range(count):
        drain(pool[q].at[pl.ds(0, (n_head - 1) * slots)], b_xsend.at[q])
        drain(ordered[q].at[pl.ds(0, n_seq - 1)], b_send.at[q])
    drain(far1, s_send.at[0])
    drain(near1.at[pl.ds(0, near - 1)], s_send.at[1])
    drain(row1.at[pl.ds(0, blocks - 1)], s_send.at[2])
    drain(tile3.at[pl.ds(0, n_kv - 1)], s_send.at[3])
    drain(state4.at[pl.ds(0, n_kv - 1)], s_send.at[4])
    drain(swap5, s_send.at[5])
    drain(ag5.at[pl.ds(0, blocks - 1)], s_send.at[6])
    drain(ag5.at[pl.ds(0, (near - 1) * blocks)], s_send.at[7])
    drain(part6.at[pl.ds(0, n_head - 1)], s_send.at[8])
    drain(far7, s_send.at[9])
    drain(near8.at[pl.ds(0, near - 1)], s_send.at[10])
    drain(row8.at[pl.ds(0, blocks - 1)], s_send.at[11])
    drain(ag9.at[pl.ds(0, blocks - 1)], s_send.at[12])
    drain(ag9.at[pl.ds(0, (near - 1) * blocks)], s_send.at[13])
    drain(ag9, s_send.at[14])
    drain(part11.at[pl.ds(0, n_head - 1)], s_send.at[15])


def angle_table(positions):
    turns = np.exp(np.arange(HD // 2) * (-2.0 * ROPE_LOG / HD))
    angles = positions[:, None] * np.concatenate([turns, turns])[None, :]
    return jnp.asarray(np.stack([np.cos(angles), np.sin(angles)], axis=1), F32)


def shards(
    tokens,
    attn_gain,
    ffn_gain,
    w_query,
    w_key,
    w_value,
    w_out,
    w_gate,
    w_up,
    w_down,
    kv_pool,
    lengths,
    pool_row,
    block_table,
):
    rows, features = tokens.shape
    n_seq, n_head, n_rep = (lax.axis_size(a) for a in ("seq", "head", "rep"))
    slots, half = kv_pool.shape[2:4]
    width = kv_pool.shape[4] // n_head
    n_kv = n_head * n_rep

    given = (
        tokens,
        pool_row[None, :],
        attn_gain[None, :],
        ffn_gain[None, :],
        angle_table(np.arange(BLK * block_table.shape[1] // STEP + 1) * STEP),
        angle_table(np.arange(STEP)),
        w_query,
        w_key,
        w_value,
        kv_pool,
        w_out.T,
        w_gate,
        w_up,
        w_down.T,
        block_table,
        pool_row,
        lengths,
    )
    vmem = pl.BlockSpec(memory_space=pltpu.VMEM)
    hbm = pl.BlockSpec(memory_space=pltpu.HBM)
    pieces, near = PIECES, 4
    rounds = (n_seq // (2 * near)).bit_length() - 1
    blocks = n_seq // near
    pool = (n_head * slots, half // pieces, width)
    ring = (n_seq, half // pieces, width)
    line, lines = (rows, 8, HD), (rows, 16, HD)
    return pl.pallas_call(
        functools.partial(kernel, n_seq, n_head, n_rep, near, pieces),
        out_shape=(
            jax.ShapeDtypeStruct((rows, features), BF16),
            jax.ShapeDtypeStruct((2, rows, half, width), BF16),
        ),
        in_specs=[hbm] * len(given),
        out_specs=(vmem, vmem),
        scratch_shapes=[
            *(pltpu.VMEM(a.shape, a.dtype) for a in given[:9]),
            pltpu.VMEM((2, *kv_pool.shape[2:]), BF16),
            *(pltpu.VMEM(a.shape, a.dtype) for a in given[10:14]),
            *(pltpu.SMEM(a.shape, a.dtype) for a in given[14:]),
            *(pltpu.VMEM(pool, BF16) for _ in range(2 * pieces)),
            *(pltpu.VMEM(ring, BF16) for _ in range(4 * pieces)),
            *(pltpu.VMEM(line, F32) for _ in range(3)),
            pltpu.VMEM((near, blocks, 8, HD), F32),
            pltpu.VMEM((blocks, 8, HD), F32),
            pltpu.VMEM((blocks, 8, HD), F32),
            pltpu.VMEM((n_kv, 8, HD), F32),
            pltpu.VMEM((n_kv, 16, HD), F32),
            pltpu.VMEM((n_kv, 16, HD), F32),
            pltpu.VMEM((8, HD), F32),
            pltpu.VMEM((8, HD), F32),
            pltpu.VMEM(line, BF16),
            pltpu.VMEM(line, F32),
            pltpu.VMEM((n_head, rows, HD), F32),
            *(pltpu.VMEM(lines, F32) for _ in range(3)),
            pltpu.VMEM(lines, BF16),
            pltpu.VMEM((near, blocks, 16, HD), BF16),
            pltpu.VMEM((blocks, 16, HD), F32),
            pltpu.VMEM((blocks, 16, HD), BF16),
            pltpu.VMEM((blocks, 16, HD), BF16),
            *(pltpu.VMEM(line, BF16) for _ in range(2)),
            pltpu.VMEM((n_head, rows, HD), F32),
            pltpu.SemaphoreType.DMA((16,)),
            pltpu.SemaphoreType.DMA((16,)),
            pltpu.SemaphoreType.DMA((len(given),)),
            *(pltpu.SemaphoreType.DMA((2 * pieces,)) for _ in range(4)),
            pltpu.SemaphoreType.REGULAR((rounds,)),
        ],
        compiler_params=pltpu.CompilerParams(
            collective_id=0, has_side_effects=True, vmem_limit_bytes=40 * 1024 * 1024
        ),
        name="decode_layer",
    )(*(pltpu.with_memory_space_constraint(a, pltpu.HBM) for a in given))


def solution(mesh):
    in_specs = (
        P("groups", ("seq", "rep")),
        P(("seq", "rep")),
        P(("seq", "rep")),
        P(("seq", "rep"), "head"),
        P(("seq", "rep"), "head"),
        P(("seq", "rep"), "head"),
        P("head", ("seq", "rep")),
        P(("seq", "rep"), "head"),
        P(("seq", "rep"), "head"),
        P("head", ("seq", "rep")),
        P(None, ("groups", "seq"), "head", "rep", None),
        P("groups"),
        P("groups"),
        P("groups", None),
    )
    out_specs = (P("groups", ("seq", "rep")), P(None, "groups", ("seq", "rep"), "head"))
    return jax.shard_map(shards, mesh=mesh, in_specs=in_specs, out_specs=out_specs, check_vma=False)
```
